32 devices in a mesh: pulse: 8 (over z, core), range: 4 (over y, x).
Axes of the slice: x: 2, y: 2, z: 4, core: 2. Of those that a mesh axis runs over, the one named last changes fastest.
Arguments:
- pulse_data: bfloat16 [2, 8192, 4096], P(None, 'pulse', 'range'), may hold values from -6 to 6
- merge_taps: int32 [3, 2, 4, 8192], P(None, None, None, 'pulse'), may hold values from 0 to 1023, as said below
- merge_weights: bfloat16 [3, 2, 4, 8192], P(None, None, None, 'pulse'), may hold values from -2 to 2
- squint: float32 [3, 8192], P(None, 'pulse'), may hold values from -8 to 8
Outputs:
- focused: float32 [2, 1024, 4096], P(None, 'pulse', 'range')
The draws below stay inside these ranges and needn't reach their ends.
Inputs may be any that keep to these rules, and one draw needn't show every extreme that they name: `merge_taps`: for each level, source half and output beam, the 4 taps name different beams of the source block.
All inputs are finite; a program needn't handle non-finite values.
Results may differ from the reference program's by a relative error of at most 0.0064.
Values may be sent and summed in bfloat16 or wider, within the bound.
No kernel may reach another device: no remote copies, remote signals or barrier semaphores. Data moves between devices by JAX's collectives and lax.ppermute only.
A program may use at most 64 MiB of HBM per device.

```python
import math
import jax
import jax.numpy as jnp
import numpy as np
from jax import lax

BEAM_DEV = 1024
RANGES = 4096
BINS = 1024
BLOCK = 64
TAPS = 4
LEVELS = 3
POWER = 3
ANGLES = 8192
N_PULSE = 8


def draw_merge_taps(key, part):
    spread = BEAM_DEV // TAPS
    base = jax.random.randint(jax.random.fold_in(key, 11), (LEVELS, 2, 1, ANGLES), 0, BEAM_DEV)
    jitter = jax.random.randint(jax.random.fold_in(key, 12), (LEVELS, 2, TAPS, ANGLES), 0, spread)
    order = lax.broadcasted_iota(jnp.int32, (LEVELS, 2, TAPS, ANGLES), 2)
    offset = jnp.where(order == 0, 0, order * spread + jitter)
    return ((base + offset) % BEAM_DEV).astype(jnp.int32)


def levels(rng, shape, shards, low, largest):
    def one(axis_at, shards_of):
        heights = jax.random.uniform(jax.random.fold_in(jax.random.fold_in(rng, 6), axis_at), (shards_of,), jnp.float32, low / len(shards), largest / len(shards))
        return jnp.repeat(jnp.exp(heights), shape[axis_at] // shards_of).reshape((-1,) + (1,) * (len(shape) - axis_at - 1))

    gain = one(*shards[0])
    for cut in shards[1:]:
        gain = gain * one(*cut)
    return gain


def noise(key, extent, deviation, reach, pieces=(), held_as=jnp.bfloat16):
    loudness = levels(key, extent, pieces, -0.22, 0.18) if pieces else 1.0
    entries = jax.random.normal(key, extent, jnp.float32) * deviation * loudness
    return jnp.minimum(jnp.maximum(entries, -reach), reach).astype(held_as)


def setup_inputs(seed: int = 0) -> dict:
    key_of = jax.random.split(jax.random.key(seed), 5)
    pulse_data = noise(key_of[0], (2, ANGLES, RANGES), 1.0, 6.0, ((1, 8), (2, 4)))
    merge_taps = draw_merge_taps(jax.random.fold_in(key_of[4], 71), 0)
    merge_weights = noise(key_of[2], (LEVELS, 2, TAPS, ANGLES), 0.35, 2.0, ((3, 8),))
    squint = jnp.clip(jax.random.uniform(key_of[3], (LEVELS, ANGLES), jnp.float32, -8.0, 8.0) * levels(key_of[3], (LEVELS, ANGLES), ((1, 8),), -0.4, 0.0), -8.0, 8.0)
    return dict(pulse_data=pulse_data, merge_taps=merge_taps, merge_weights=merge_weights, squint=squint)


TWO_PI = 2.0 * math.pi
EPSILON = 1e-06

def merge_all(pulse_data, merge_taps, merge_weights, squint):
    data = pulse_data.reshape(2, N_PULSE, BEAM_DEV, RANGES).transpose(1, 0, 2, 3)
    range_phase = jnp.arange(RANGES, dtype=jnp.int32).astype(jnp.float32) * (TWO_PI / RANGES)

    def merge_block(items):
        own, other, taps_block, weights_block, squint_block = items
        total = jnp.zeros(own.shape, jnp.float32)
        for source, block in ((0, own), (1, other)):
            for tap in range(TAPS):
                picked = jnp.take(block, taps_block[source, tap], axis=1).astype(jnp.float32)
                total = total + weights_block[source, tap].astype(jnp.float32)[None, :, None] * picked
        phase = squint_block[:, None] * range_phase[None, :]
        cosine = jnp.cos(phase)
        sine = jnp.sin(phase)
        real = cosine * total[0] - sine * total[1]
        imag = sine * total[0] + cosine * total[1]
        return jnp.stack([real, imag]).astype(jnp.bfloat16)
    for level in range(LEVELS):
        partner_order = np.arange(N_PULSE) ^ 1 << level
        other = data[partner_order]
        taps_level = merge_taps[level].reshape(2, TAPS, N_PULSE, BEAM_DEV).transpose(2, 0, 1, 3)
        weights_level = merge_weights[level].reshape(2, TAPS, N_PULSE, BEAM_DEV).transpose(2, 0, 1, 3)
        squint_level = squint[level].reshape(N_PULSE, BEAM_DEV)
        data = lax.map(merge_block, (data, other, taps_level, weights_level, squint_level))
    return data.transpose(1, 0, 2, 3).reshape(2, ANGLES, RANGES)

def reference(pulse_data, merge_taps, merge_weights, squint):
    beams = merge_all(pulse_data, merge_taps, merge_weights, squint).astype(jnp.float32)
    bins_col = jnp.arange(BINS, dtype=jnp.int32)[:, None]
    angle_row = jnp.arange(ANGLES, dtype=jnp.int32)[None, :]
    theta = (bins_col * angle_row % ANGLES).astype(jnp.float32) * (TWO_PI / ANGLES)
    cosine = jnp.cos(theta).astype(jnp.bfloat16).astype(jnp.float32)
    sine = jnp.sin(theta).astype(jnp.bfloat16).astype(jnp.float32)
    along_cos = jnp.einsum('fa,tar->ftr', cosine, beams)
    along_sin = jnp.einsum('fa,tar->ftr', sine, beams)
    scale = ANGLES ** (-0.5)
    spec_re = (along_cos[:, 0] + along_sin[:, 1]) * scale
    spec_im = (along_cos[:, 1] - along_sin[:, 0]) * scale
    blocks = BINS // BLOCK
    g_re = spec_re.reshape(blocks, BLOCK, RANGES)
    g_im = spec_im.reshape(blocks, BLOCK, RANGES)
    highest = lax.Precision.HIGHEST
    cov_re = jnp.einsum('bjr,bkr->bjk', g_re, g_re, precision=highest) + jnp.einsum('bjr,bkr->bjk', g_im, g_im, precision=highest)
    cov_im = jnp.einsum('bjr,bkr->bjk', g_im, g_re, precision=highest) - jnp.einsum('bjr,bkr->bjk', g_re, g_im, precision=highest)
    vec_re = jnp.ones((blocks, BLOCK), jnp.float32)
    vec_im = jnp.zeros((blocks, BLOCK), jnp.float32)
    for step in range(POWER):
        new_re = jnp.einsum('bjk,bk->bj', cov_re, vec_re, precision=highest) - jnp.einsum('bjk,bk->bj', cov_im, vec_im, precision=highest)
        new_im = jnp.einsum('bjk,bk->bj', cov_re, vec_im, precision=highest) + jnp.einsum('bjk,bk->bj', cov_im, vec_re, precision=highest)
        length = jnp.sqrt(lax.optimization_barrier(jnp.sum(new_re * new_re + new_im * new_im, axis=1, keepdims=True)) + EPSILON)
        vec_re = new_re / length
        vec_im = new_im / length
    factor = math.sqrt(BLOCK)
    out_re = (g_re * vec_re[:, :, None] + g_im * vec_im[:, :, None]) * factor
    out_im = (g_im * vec_re[:, :, None] - g_re * vec_im[:, :, None]) * factor
    return jnp.stack([out_re.reshape(BINS, RANGES), out_im.reshape(BINS, RANGES)])
```

```python
import functools
import math

import jax
import jax.numpy as jnp
from jax import lax
from jax.experimental import pallas as pl
from jax.experimental.pallas import tpu as pltpu
from jax.sharding import PartitionSpec as P

BINS = 1024
BLOCK = 64
LEVELS = 3
POWER = 3
CALLS = 2
LANES = 128
EPSILON = 1e-06


F32 = jnp.float32
BF16 = jnp.bfloat16


def cis_turns(turns):
    x = (turns - jnp.floor(turns + 0.5)) * math.pi
    y = x * x
    s = 1.0 / 362880 - y * (1.0 / 39916800)
    s = -1.0 / 5040 + y * s
    s = 1.0 / 120 + y * s
    s = -1.0 / 6 + y * s
    s = x * (1.0 + y * s)
    c = 1.0 / 40320 - y * (1.0 / 3628800)
    c = -1.0 / 720 + y * c
    c = 1.0 / 24 + y * c
    c = -1.0 / 2 + y * c
    c = 1.0 + y * c
    return 1.0 - 2.0 * s * s, 2.0 * s * c


def swap(block, axis, distance):
    count = lax.axis_size(axis)
    return lax.ppermute(block, axis, [(i, i ^ distance) for i in range(count)])


SQUINTS = 64
BIN_COL = 71
ANGLE_COL = 72
RANGE_COL = 73
COLUMNS = 80


def prep_kernel(angles, params, matrices, table):
    rows = params.shape[0]
    width = matrices.shape[2]
    step = 32

    def part(i, _):
        at = pl.ds(pl.multiple_of(i * step, step), step)
        p = params[at, :]
        columns = lax.broadcasted_iota(jnp.int32, (step, width), 1).astype(F32)
        for unit in range(8):
            total = jnp.zeros((step, width), F32)
            for tap in range(4):
                where = p[:, 8 * unit + tap : 8 * unit + tap + 1]
                weight = p[:, 8 * unit + 4 + tap : 8 * unit + 5 + tap]
                total = jnp.where(columns == where, weight, total)
            matrices[unit, at, :] = total.astype(BF16)
        bins = p[:, BIN_COL : BIN_COL + 1].astype(jnp.int32)
        first = p[:, ANGLE_COL : ANGLE_COL + 1].astype(jnp.int32)
        lane = lax.broadcasted_iota(jnp.int32, (step, LANES), 1)
        fine_c, fine_s = cis_turns(lax.rem(bins * lane, angles).astype(F32) * (1.0 / angles))
        coarse_c, coarse_s = cis_turns(
            lax.rem(bins * lax.rem(first + lane * LANES, angles), angles).astype(F32)
            * (1.0 / angles)
        )
        for j in range(width // LANES):
            a_c = coarse_c[:, j : j + 1]
            a_s = coarse_s[:, j : j + 1]
            table[at, j * LANES : (j + 1) * LANES] = (a_c * fine_c - a_s * fine_s).astype(BF16)
            table[at, width + j * LANES : width + (j + 1) * LANES] = (
                a_s * fine_c + a_c * fine_s
            ).astype(BF16)
        return 0

    lax.fori_loop(0, rows // step, part, 0)


def prepare(params, angles):
    beams = params.shape[0]
    rows = 128
    return pl.pallas_call(
        functools.partial(prep_kernel, angles),
        grid=(beams // rows,),
        in_specs=[pl.BlockSpec((rows, COLUMNS), lambda i: (i, 0))],
        out_specs=[
            pl.BlockSpec((8, rows, beams), lambda i: (0, i, 0)),
            pl.BlockSpec((rows, 2 * beams), lambda i: (i, 0)),
        ],
        out_shape=[
            jax.ShapeDtypeStruct((8, beams, beams), BF16),
            jax.ShapeDtypeStruct((BINS, 2 * beams), BF16),
        ],
        cost_estimate=pl.CostEstimate(
            flops=20 * 8 * beams * beams, bytes_accessed=20 * beams * beams, transcendentals=0
        ),
        name="prep",
    )(params)


def main_kernel(
    part, ranges, classes,
    params, own_hbm, other_hbm, mat_hbm, table_hbm,
    keep, send,
    own, other, mat, azimuth, phase, step, merged, pair, spread, sems,
):
    beams = own.shape[1]
    width = own.shape[2]
    tile = 256
    tiles = beams // tile
    copies = [
        pltpu.make_async_copy(own_hbm.at[:, :, pl.ds(part * width, width)], own, sems.at[0]),
        pltpu.make_async_copy(mat_hbm.at[pl.ds(0, 2)], mat.at[pl.ds(0, 2)], sems.at[1]),
        pltpu.make_async_copy(other_hbm.at[:, :, pl.ds(part * width, width)], other, sems.at[2]),
        pltpu.make_async_copy(mat_hbm.at[pl.ds(2, 2)], mat.at[pl.ds(2, 2)], sems.at[3]),
        pltpu.make_async_copy(mat_hbm.at[pl.ds(4, 4)], mat.at[pl.ds(4, 4)], sems.at[4]),
        pltpu.make_async_copy(table_hbm, azimuth, sems.at[5]),
    ]
    for copy in copies:
        copy.start()

    def begin(i, _):
        at = pl.ds(pl.multiple_of(i * 64, 64), 64)
        p = params[at, :]
        lane = lax.broadcasted_iota(jnp.int32, (64, LANES), 1).astype(F32)
        index = (p[:, RANGE_COL : RANGE_COL + 1] + (lane + part * width)) * (1.0 / ranges)
        for unit in range(7):
            squint = p[:, SQUINTS + unit : SQUINTS + unit + 1]
            cosine, sine = cis_turns(squint * index)
            phase[unit, 0, at, :] = cosine
            phase[unit, 1, at, :] = sine
        cosine, sine = cis_turns(p[:, SQUINTS : SQUINTS + 8] * (LANES / ranges))
        step[at, 0:8] = cosine
        step[at, 8:16] = sine
        return 0

    lax.fori_loop(0, beams // 64, begin, 0)

    def rotate(unit, at, total):
        cosine = phase[unit, 0, at, :]
        sine = phase[unit, 1, at, :]
        if width > LANES:
            ahead_c = step[at, unit : unit + 1]
            ahead_s = step[at, 8 + unit : 9 + unit]
            phase[unit, 0, at, :] = cosine * ahead_c - sine * ahead_s
            phase[unit, 1, at, :] = cosine * ahead_s + sine * ahead_c
        real = total[:, :LANES]
        imag = total[:, LANES:]
        return cosine * real - sine * imag, sine * real + cosine * imag

    def product(lhs, rhs):
        return jnp.dot(lhs, rhs, preferred_element_type=F32)

    def wait(j, *which):
        @pl.when(j == 0)
        def _():
            for i in which:
                copies[i].wait()

    def chunk(j, _):
        lanes = pl.ds(pl.multiple_of(j * LANES, LANES), LANES)
        wait(j, 0, 1, 2)
        near = jnp.concatenate([own[0, :, lanes], own[1, :, lanes]], axis=1)
        far = jnp.concatenate([other[0, :, lanes], other[1, :, lanes]], axis=1)
        for i in range(tiles):
            at = pl.ds(i * tile, tile)
            real, imag = rotate(0, at, product(mat[0, at, :], near) + product(mat[1, at, :], far))
            merged[at, :LANES] = real.astype(BF16)
            merged[at, LANES:] = imag.astype(BF16)
        wait(j, 3)
        for x in range(2):
            for i in range(tiles):
                at = pl.ds(i * tile, tile)
                real, imag = rotate(1 + x, at, product(mat[2 + x, at, :], merged[...]))
                pair[x, at, :LANES] = real.astype(BF16)
                pair[x, at, LANES:] = imag.astype(BF16)
        wait(j, 4)
        for i in range(tiles):
            at = pl.ds(i * tile, tile)
            low = pl.ds(beams + i * tile, tile)
            terms = [
                rotate(3 + k, at, product(mat[4 + k, at, :], pair[k % 2])) for k in range(4)
            ]
            for q in range(classes):
                real = terms[0][0]
                imag = terms[0][1]
                for k in range(1, 4):
                    turn = (q * k) % classes
                    c = math.cos(2.0 * math.pi * turn / classes)
                    s = math.sin(2.0 * math.pi * turn / classes)
                    c = float(round(c)) if abs(c - round(c)) < 1e-9 else c
                    s = float(round(s)) if abs(s - round(s)) < 1e-9 else s
                    re, im = terms[k]
                    for amount, add_re, add_im in ((c, re, im), (s, im, -re)):
                        if amount == 1.0:
                            real, imag = real + add_re, imag + add_im
                        elif amount == -1.0:
                            real, imag = real - add_re, imag - add_im
                        elif amount != 0.0:
                            real, imag = real + amount * add_re, imag + amount * add_im
                real_b = real.astype(BF16)
                imag_b = imag.astype(BF16)
                spread[q, at, :LANES] = real_b
                spread[q, at, LANES:] = imag_b
                spread[q, low, :LANES] = imag_b
                spread[q, low, LANES:] = -real_b
        wait(j, 5)
        rows = BINS // classes
        half = rows // 2
        for q in range(classes):
            result = product(azimuth[pl.ds(q * rows, rows), :], spread[q])
            for t in range(2):
                side = result[:, t * LANES : (t + 1) * LANES]
                keep[t, q, :, lanes] = side[:half]
                send[t, q, :, lanes] = side[half:].astype(BF16)
        return 0

    lax.fori_loop(0, width // LANES, chunk, 0)


def partial_spectrum(part, params, own, other, matrices, table, ranges, classes):
    beams = own.shape[1]
    width = own.shape[2] // CALLS
    half = BINS // classes // 2
    vmem = pl.BlockSpec(memory_space=pltpu.VMEM)
    hbm = pl.BlockSpec(memory_space=pl.ANY)
    return pl.pallas_call(
        functools.partial(main_kernel, part, ranges, classes),
        in_specs=[vmem, hbm, hbm, hbm, hbm],
        out_specs=[vmem, vmem],
        out_shape=[
            jax.ShapeDtypeStruct((2, classes, half, width), F32),
            jax.ShapeDtypeStruct((2, classes, half, width), BF16),
        ],
        scratch_shapes=[
            pltpu.VMEM((2, beams, width), BF16),
            pltpu.VMEM((2, beams, width), BF16),
            pltpu.VMEM((8, beams, beams), BF16),
            pltpu.VMEM((BINS, 2 * beams), BF16),
            pltpu.VMEM((7, 2, beams, LANES), F32),
            pltpu.VMEM((beams, 16), F32),
            pltpu.VMEM((beams, 2 * LANES), BF16),
            pltpu.VMEM((2, beams, 2 * LANES), BF16),
            pltpu.VMEM((classes, 2 * beams, 2 * LANES), BF16),
            pltpu.SemaphoreType.DMA((6,)),
        ],
        compiler_params=pltpu.CompilerParams(vmem_limit_bytes=62 * 1024 * 1024),
        cost_estimate=pl.CostEstimate(
            flops=2 * 20 * beams * beams * width,
            bytes_accessed=26 * beams * beams,
            transcendentals=0,
        ),
        name="main",
    )(params, own, other, matrices, table)


def covariance_kernel(scale, *refs):
    parts = (len(refs) - 2) // 2
    kept, received = refs[:parts], refs[parts : 2 * parts]
    spectrum, covariance = refs[2 * parts :]
    classes, rows = kept[0].shape[1:3]
    width = kept[0].shape[3]
    inner = BLOCK // classes
    for h in range(parts):
        spectrum[:, :, :, h * width : (h + 1) * width] = (
            kept[h][...] + received[h][...].astype(F32)
        ) * scale

    def gram(a, b):
        return lax.dot_general(
            a, b, (((1,), (1,)), ((), ())),
            precision=lax.Precision.HIGHEST, preferred_element_type=F32,
        )

    for b in range(rows // inner):
        real, imag = [
            jnp.concatenate(
                [spectrum[t, q, b * inner : (b + 1) * inner, :] for q in range(classes)], axis=0
            )
            for t in range(2)
        ]
        covariance[b] = gram(real, jnp.concatenate([real, -imag], axis=0)) + gram(
            imag, jnp.concatenate([imag, real], axis=0)
        )


def spectrum_and_covariance(kept, received, scale):
    _, classes, rows, width = kept[0].shape
    inner = BLOCK // classes
    vmem = pl.BlockSpec(memory_space=pltpu.VMEM)
    return pl.pallas_call(
        functools.partial(covariance_kernel, scale),
        in_specs=[vmem] * (2 * len(kept)),
        out_specs=[vmem, vmem],
        out_shape=[
            jax.ShapeDtypeStruct((2, classes, rows, width * len(kept)), F32),
            jax.ShapeDtypeStruct((rows // inner, BLOCK, 2 * BLOCK), F32),
        ],
        name="covariance",
    )(*kept, *received)


def focus_kernel(*refs):
    covs, (spectrum, out, stage) = refs[:-3], refs[-3:]
    classes, rows = spectrum.shape[1:3]
    inner = BLOCK // classes
    factor = math.sqrt(BLOCK)
    lane = lax.broadcasted_iota(jnp.int32, (1, 2 * BLOCK), 1)
    first = lane < BLOCK

    def turned(row):
        return pltpu.roll(jnp.broadcast_to(row, (8, 2 * BLOCK)), BLOCK, 1)[0:1]

    for b in range(rows // inner):
        cov = covs[0][b]
        for other in covs[1:]:
            cov = cov + other[b]
        vec_re = jnp.where(first, 1.0, 0.0)
        vec_im = jnp.zeros((1, 2 * BLOCK), F32)
        for step in range(POWER):
            if step % 2 == 0:
                new_re = jnp.sum(
                    cov * jnp.where(first, vec_re, -turned(vec_im)), axis=1, keepdims=True
                )
                new_im = jnp.sum(
                    cov * jnp.where(first, vec_im, turned(vec_re)), axis=1, keepdims=True
                )
                power = jnp.sum(new_re * new_re + new_im * new_im, axis=0, keepdims=True)
            else:
                by_re = jnp.sum(cov * vec_re, axis=0, keepdims=True)
                by_im = jnp.sum(cov * vec_im, axis=0, keepdims=True)
                new_re = jnp.where(first, by_re + turned(by_im), 0.0)
                new_im = jnp.where(first, by_im - turned(by_re), 0.0)
                power = jnp.sum(new_re * new_re + new_im * new_im, axis=1, keepdims=True)
            length = jnp.sqrt(power + EPSILON)
            vec_re = new_re / length
            vec_im = new_im / length
        for q in range(classes):
            re = spectrum[0, q, b * inner : (b + 1) * inner, :]
            im = spectrum[1, q, b * inner : (b + 1) * inner, :]
            by_re = vec_re[q * inner : (q + 1) * inner] * factor
            by_im = vec_im[q * inner : (q + 1) * inner] * factor
            at = pl.ds(q, inner, stride=classes)
            for t, side in enumerate((re * by_re + im * by_im, im * by_re - re * by_im)):
                for j in range(stage.shape[1]):
                    stage[t, j, at, :] = side[:, j * LANES : (j + 1) * LANES]
        for t in range(2):
            for j in range(stage.shape[1]):
                out[t, b * BLOCK : (b + 1) * BLOCK, j * LANES : (j + 1) * LANES] = stage[t, j]


def focus(covs, spectrum):
    _, classes, rows, ranges = spectrum.shape
    vmem = pl.BlockSpec(memory_space=pltpu.VMEM)
    return pl.pallas_call(
        focus_kernel,
        in_specs=[vmem] * (len(covs) + 1),
        out_specs=vmem,
        out_shape=jax.ShapeDtypeStruct((2, classes * rows, ranges), F32),
        scratch_shapes=[pltpu.VMEM((2, ranges // LANES, BLOCK, LANES), F32)],
        name="focus",
    )(*covs, spectrum)


def parameters(merge_taps, merge_weights, squint, range_cols, beams, pulses):
    pulse_index = lax.axis_index("pulse")
    range_index = lax.axis_index("range")
    taps = merge_taps.astype(F32)
    weights = merge_weights.astype(F32)

    def rows(level, source):
        return jnp.concatenate(
            [taps[level, source], weights[level, source], squint[level][None]], axis=0
        )

    mine = [rows(1, 0), rows(2, 0)]
    near = swap(jnp.concatenate([rows(1, 1), rows(2, 0)], axis=0), "pulse", 2)
    middle = swap(rows(2, 1), "pulse", 4)
    far = swap(rows(2, 1), "pulse", 6)
    place = pulse_index >> 1 & 3
    first = jnp.stack([mine[0], near[:9]])
    second = jnp.stack([mine[1], near[9:], middle, far])
    first = [lax.dynamic_index_in_dim(first, x ^ place & 1, 0, False) for x in range(2)]
    second = [lax.dynamic_index_in_dim(second, k ^ place, 0, False) for k in range(4)]
    units = [rows(0, 0), rows(0, 1)] + first + second
    classes = pulses // 2
    count = pulses * (BINS // pulses // classes)
    row = lax.iota(jnp.int32, BINS)
    group = row % count // (BINS // pulses // classes)
    reversed_group = jnp.zeros_like(group)
    bits = pulses.bit_length() - 1
    for bit in range(bits):
        reversed_group = reversed_group | (group >> bit & 1) << bits - 1 - bit
    bins = (
        (reversed_group ^ pulse_index) * (BINS // pulses)
        + row % (BINS // pulses // classes) * classes
        + row // count
    )
    whole = lambda value: jnp.full((1, beams), value, F32)
    stacked = jnp.concatenate(
        [unit[:8] for unit in units]
        + [unit[8:] for unit in [units[0]] + first + second]
        + [
            bins.astype(F32)[None],
            whole((pulse_index & ~6) * beams),
            whole(range_index * range_cols),
            jnp.zeros((COLUMNS - RANGE_COL - 1, beams), F32),
        ],
        axis=0,
    )
    return stacked.T


def per_device(pulse_data, merge_taps, merge_weights, squint):
    pulses = lax.axis_size("pulse")
    range_count = lax.axis_size("range")
    _, beams, range_cols = pulse_data.shape
    ranges = range_cols * range_count
    angles = beams * pulses
    classes = pulses // 2
    other = swap(pulse_data, "pulse", 1)
    params = parameters(merge_taps, merge_weights, squint, range_cols, beams, pulses)
    matrices, table = prepare(params, angles)
    kept, received = [], []
    for part in range(CALLS):
        keep, send = partial_spectrum(
            part, params, pulse_data, other, matrices, table, ranges, classes
        )
        distance = 1
        while True:
            arrived = swap(send, "pulse", distance)
            distance *= 2
            if distance == pulses:
                break
            total = keep + arrived.astype(F32)
            half = total.shape[2] // 2
            keep = total[:, :, :half]
            send = total[:, :, half:].astype(BF16)
        kept.append(keep)
        received.append(arrived)
    spectrum, cov = spectrum_and_covariance(kept, received, angles ** (-0.5))
    covs = [cov]
    distance = 1
    while distance < range_count:
        total = covs[0]
        for extra in covs[1:]:
            total = total + extra
        covs = [total]
        for turn in range(1, min(4, range_count // distance)):
            covs.append(swap(total, "range", turn * distance))
        distance *= 4
    return focus(covs, spectrum)


def solution(mesh):
    placed = (
        P(None, "pulse", "range"),
        P(None, None, None, "pulse"),
        P(None, None, None, "pulse"),
        P(None, "pulse"),
    )
    return jax.shard_map(
        per_device, mesh=mesh, in_specs=placed, out_specs=P(None, "pulse", "range"), check_vma=False
    )
```

```python
import functools
import math

import jax
import jax.numpy as jnp
from jax import lax
from jax.experimental import pallas as pl
from jax.experimental.pallas import tpu as pltpu
from jax.sharding import PartitionSpec as P


BINS = 1024
BLOCK = 64
POWER = 3
CALLS = 4
MIB = 1024 * 1024
SMALL_LIMIT = 4
LANES = 128
EPSILON = 1e-06


F32 = jnp.float32
BF16 = jnp.bfloat16


def cis_turns(turns):
    x = (turns - jnp.floor(turns + 0.5)) * math.pi
    y = x * x
    s = 1.0 / 362880 - y * (1.0 / 39916800)
    s = -1.0 / 5040 + y * s
    s = 1.0 / 120 + y * s
    s = -1.0 / 6 + y * s
    s = x * (1.0 + y * s)
    c = 1.0 / 40320 - y * (1.0 / 3628800)
    c = -1.0 / 720 + y * c
    c = 1.0 / 24 + y * c
    c = -1.0 / 2 + y * c
    c = 1.0 + y * c
    return 1.0 - 2.0 * s * s, 2.0 * s * c


def swap(block, axis, distance):
    count = lax.axis_size(axis)
    return lax.ppermute(block, axis, [(i, i ^ distance) for i in range(count)])


VMEM = pl.BlockSpec(memory_space=pltpu.VMEM)
SMEM = pl.BlockSpec(memory_space=pltpu.SMEM)
HBM = pl.BlockSpec(memory_space=pl.ANY)


def pack_kernel(taps, weights, squint, mine, near, far):
    def put(out, row, level, source):
        out[row : row + 4] = taps[level, source].astype(F32)
        out[row + 4 : row + 8] = weights[level, source].astype(F32)

    put(mine, 0, 0, 0)
    put(mine, 8, 0, 1)
    put(mine, 16, 1, 0)
    put(mine, 24, 2, 0)
    mine[32:35] = squint[...]
    mine[35:40] = jnp.zeros((5, mine.shape[1]), F32)
    put(near, 0, 1, 1)
    put(near, 8, 2, 0)
    near[16:19] = squint[...]
    near[19:24] = jnp.zeros((5, near.shape[1]), F32)
    put(far, 0, 2, 1)
    far[8:11] = squint[...]
    far[11:16] = jnp.zeros((5, far.shape[1]), F32)


def pack(taps, weights, squint):
    beams = squint.shape[1]
    return pl.pallas_call(
        pack_kernel,
        in_specs=[VMEM] * 3,
        out_specs=[VMEM] * 3,
        out_shape=[jax.ShapeDtypeStruct((rows, beams), F32) for rows in (40, 24, 16)],
        compiler_params=pltpu.CompilerParams(vmem_limit_bytes=SMALL_LIMIT * MIB),
        name="pack",
    )(taps, weights, squint)


def fill_matrices(columns, outs):
    beams = columns.shape[0]

    def part(i, _):
        at = pl.ds(pl.multiple_of(i * 16, 16), 16)
        lane = lax.broadcasted_iota(jnp.int32, (8, LANES), 1).astype(F32)
        for unit, out in enumerate(outs):
            halves = []
            for h in range(2):
                p = columns[pl.ds(pl.multiple_of(i * 16 + 8 * h, 8), 8), :]
                spread = [
                    jnp.broadcast_to(p[:, 8 * unit + c : 8 * unit + c + 1], (8, LANES))
                    for c in range(8)
                ]
                halves.append(spread)
            for j in range(beams // LANES):
                totals = []
                for spread in halves:
                    total = jnp.zeros((8, LANES), F32)
                    for tap in range(4):
                        total = jnp.where(lane + j * LANES == spread[tap], spread[4 + tap], total)
                    totals.append(total)
                out[at, j * LANES : (j + 1) * LANES] = jnp.concatenate(
                    totals, axis=0
                ).astype(BF16)
        return 0

    lax.fori_loop(0, beams // 16, part, 0)


def first_kernel(pulses, scalars, mine, matrices, table, columns, rows):
    beams = matrices.shape[1]
    angles = beams * pulses
    classes = pulses // 2
    each = BINS // pulses
    rows[0:40] = mine[...]
    columns[...] = rows[...].T
    fill_matrices(columns, [matrices.at[u] for u in range(2)])
    count = BINS // classes
    inner = each // classes
    bits = pulses.bit_length() - 1

    def part(i, _):
        at = pl.ds(pl.multiple_of(i * 16, 16), 16)
        row = lax.broadcasted_iota(jnp.int32, (16, LANES), 0) + i * 16
        group = (row & (count - 1)) >> (inner.bit_length() - 1)
        mirrored = jnp.zeros_like(group)
        for bit in range(bits):
            mirrored = mirrored | ((group >> bit & 1) << (bits - 1 - bit))
        bins = (
            (mirrored ^ scalars[0]) * each
            + (row & (inner - 1)) * classes
            + (row >> (count.bit_length() - 1))
        )
        lane = lax.broadcasted_iota(jnp.int32, (16, LANES), 1)
        whole = angles - 1
        fine_c, fine_s = cis_turns((bins * lane & whole).astype(F32) * (1.0 / angles))
        coarse_c, coarse_s = cis_turns(
            (bins * (scalars[2] + lane * LANES & whole) & whole).astype(F32) * (1.0 / angles)
        )
        for j in range(beams // LANES):
            a_c = coarse_c[:, j : j + 1]
            a_s = coarse_s[:, j : j + 1]
            table[at, j * LANES : (j + 1) * LANES] = (a_c * fine_c - a_s * fine_s).astype(BF16)
            table[at, beams + j * LANES : beams + (j + 1) * LANES] = (
                a_s * fine_c + a_c * fine_s
            ).astype(BF16)
        return 0

    lax.fori_loop(0, BINS // 16, part, 0)


def first_tables(scalars, mine, pulses):
    beams = mine.shape[1]
    return pl.pallas_call(
        functools.partial(first_kernel, pulses),
        in_specs=[SMEM, VMEM],
        out_specs=[VMEM] * 2,
        out_shape=[
            jax.ShapeDtypeStruct((2, beams, beams), BF16),
            jax.ShapeDtypeStruct((BINS, 2 * beams), BF16),
        ],
        scratch_shapes=[pltpu.VMEM((beams, LANES), F32), pltpu.VMEM((LANES, beams), F32)],
        compiler_params=pltpu.CompilerParams(vmem_limit_bytes=SMALL_LIMIT * MIB),
        cost_estimate=pl.CostEstimate(
            flops=30 * beams * beams, bytes_accessed=8 * beams * beams, transcendentals=0
        ),
        name="first",
    )(scalars, mine)


def second_kernel(ranges, scalars, mine, near, middle, far, split, join, phase, step, columns, rows, packs):
    beams = split.shape[1]
    place = scalars[1]
    packs[0, 0:8] = mine[24:32]
    packs[0, 8:16] = jnp.broadcast_to(mine[34:35], (8, beams))
    packs[1, 0:8] = near[8:16]
    packs[1, 8:16] = jnp.broadcast_to(near[18:19], (8, beams))
    packs[2, 0:8] = middle[0:8]
    packs[2, 8:16] = jnp.broadcast_to(middle[10:11], (8, beams))
    packs[3, 0:8] = far[0:8]
    packs[3, 8:16] = jnp.broadcast_to(far[10:11], (8, beams))
    packs[4, 0:8] = mine[16:24]
    packs[4, 8:16] = jnp.broadcast_to(mine[33:34], (8, beams))
    packs[5, 0:8] = near[0:8]
    packs[5, 8:16] = jnp.broadcast_to(near[17:18], (8, beams))
    order = [4 + (x ^ place & 1) for x in range(2)] + [k ^ place for k in range(4)]
    rows[48:56] = jnp.broadcast_to(mine[32:33], (8, beams))
    for unit, source in enumerate(order):
        rows[8 * unit : 8 * unit + 8] = packs[source, 0:8]
        rows[56 + 8 * unit : 64 + 8 * unit] = packs[source, 8:16]
    columns[...] = rows[...].T
    fill_matrices(
        columns, [split.at[u] for u in range(2)] + [join.at[u] for u in range(4)]
    )

    def part(i, _):
        at = pl.ds(pl.multiple_of(i * 16, 16), 16)
        p = columns[at, :]
        lane = lax.broadcasted_iota(jnp.int32, (16, LANES), 1)
        index = (lane + scalars[3]).astype(F32) * (1.0 / ranges)
        for unit in range(7):
            squint = p[:, 48 + 8 * unit : 49 + 8 * unit]
            cosine, sine = cis_turns(squint * index)
            phase[unit, 0, at, :] = cosine
            phase[unit, 1, at, :] = sine
        cosine, sine = cis_turns(p * (LANES / ranges))
        step[0, at, :] = cosine
        step[1, at, :] = sine
        return 0

    lax.fori_loop(0, beams // 16, part, 0)


def second_tables(scalars, mine, near, middle, far, ranges):
    beams = mine.shape[1]
    return pl.pallas_call(
        functools.partial(second_kernel, ranges),
        in_specs=[SMEM] + [VMEM] * 4,
        out_specs=[VMEM] * 4,
        out_shape=[
            jax.ShapeDtypeStruct((2, beams, beams), BF16),
            jax.ShapeDtypeStruct((4, beams, beams), BF16),
            jax.ShapeDtypeStruct((7, 2, beams, LANES), F32),
            jax.ShapeDtypeStruct((2, beams, LANES), F32),
        ],
        scratch_shapes=[
            pltpu.VMEM((beams, LANES), F32),
            pltpu.VMEM((LANES, beams), F32),
            pltpu.VMEM((6, 16, beams), F32),
        ],
        compiler_params=pltpu.CompilerParams(vmem_limit_bytes=SMALL_LIMIT * MIB),
        cost_estimate=pl.CostEstimate(
            flops=60 * beams * beams, bytes_accessed=12 * beams * beams, transcendentals=0
        ),
        name="second",
    )(scalars, mine, near, middle, far)


def main_limit(classes):
    return (13 if classes <= 4 else 30) * MIB


def main_kernel(
    part, classes,
    own_hbm, other_hbm, merge, split, join, azimuth, step, phase_in,
    keep, send, phase,
    own, other, merged, pair, spread, sems,
):
    beams = own.shape[2]
    width = keep.shape[3]
    tile = 512
    tiles = beams // tile

    def rotate(unit, at, total):
        cosine = phase[unit, 0, at, :]
        sine = phase[unit, 1, at, :]
        ahead_c = step[0, at, 48 + 8 * unit : 49 + 8 * unit]
        ahead_s = step[1, at, 48 + 8 * unit : 49 + 8 * unit]
        phase[unit, 0, at, :] = cosine * ahead_c - sine * ahead_s
        phase[unit, 1, at, :] = cosine * ahead_s + sine * ahead_c
        real = total[:, :LANES]
        imag = total[:, LANES:]
        return cosine * real - sine * imag, sine * real + cosine * imag

    def product(lhs, rhs):
        return jnp.dot(lhs, rhs, preferred_element_type=F32)

    def fetch(j):
        source = pl.ds(pl.multiple_of(part * width + j * LANES, LANES), LANES)
        return [
            pltpu.make_async_copy(ref.at[:, :, source], to.at[j], sems.at[i, j])
            for i, (ref, to) in enumerate(((own_hbm, own), (other_hbm, other)))
        ]

    for j in range(width // LANES):
        for copy in fetch(j):
            copy.start()

    def chunk(j, _):
        lanes = pl.ds(pl.multiple_of(j * LANES, LANES), LANES)
        for copy in fetch(j):
            copy.wait()
        near = jnp.concatenate([own[j, 0], own[j, 1]], axis=1)
        far = jnp.concatenate([other[j, 0], other[j, 1]], axis=1)
        for i in range(tiles):
            at = pl.ds(i * tile, tile)
            real, imag = rotate(
                0, at, product(merge[0, at, :], near) + product(merge[1, at, :], far)
            )
            merged[at, :LANES] = real.astype(BF16)
            merged[at, LANES:] = imag.astype(BF16)
        for x in range(2):
            for i in range(tiles):
                at = pl.ds(i * tile, tile)
                real, imag = rotate(1 + x, at, product(split[x, at, :], merged[...]))
                pair[x, at, :LANES] = real.astype(BF16)
                pair[x, at, LANES:] = imag.astype(BF16)
        for i in range(tiles):
            at = pl.ds(i * tile, tile)
            low = pl.ds(beams + i * tile, tile)
            terms = [
                rotate(3 + k, at, product(join[k, at, :], pair[k % 2])) for k in range(4)
            ]
            for q in range(classes):
                real = terms[0][0]
                imag = terms[0][1]
                for k in range(1, 4):
                    turn = (q * k) % classes
                    c = math.cos(2.0 * math.pi * turn / classes)
                    s = math.sin(2.0 * math.pi * turn / classes)
                    c = float(round(c)) if abs(c - round(c)) < 1e-9 else c
                    s = float(round(s)) if abs(s - round(s)) < 1e-9 else s
                    re, im = terms[k]
                    for amount, add_re, add_im in ((c, re, im), (s, im, -re)):
                        if amount == 1.0:
                            real, imag = real + add_re, imag + add_im
                        elif amount == -1.0:
                            real, imag = real - add_re, imag - add_im
                        elif amount != 0.0:
                            real, imag = real + amount * add_re, imag + amount * add_im
                real_b = real.astype(BF16)
                imag_b = imag.astype(BF16)
                spread[q, at, :LANES] = real_b
                spread[q, at, LANES:] = imag_b
                spread[q, low, :LANES] = imag_b
                spread[q, low, LANES:] = -real_b
        rows = BINS // classes
        half = rows // 2
        for q in range(classes):
            result = product(azimuth[pl.ds(q * rows, rows), :], spread[q])
            for t in range(2):
                side = result[:, t * LANES : (t + 1) * LANES]
                keep[t, q, :, lanes] = side[:half]
                send[t, q, :, lanes] = side[half:].astype(BF16)
        return 0

    lax.fori_loop(0, width // LANES, chunk, 0)


def partial_spectrum(part, calls, own, other, tables, phase, classes):
    beams = own.shape[1]
    width = own.shape[2] // calls
    half = BINS // classes // 2
    return pl.pallas_call(
        functools.partial(main_kernel, part, classes),
        in_specs=[HBM] * 2 + [VMEM] * 6,
        out_specs=[VMEM] * 3,
        out_shape=[
            jax.ShapeDtypeStruct((2, classes, half, width), F32),
            jax.ShapeDtypeStruct((2, classes, half, width), BF16),
            jax.ShapeDtypeStruct(phase.shape, F32),
        ],
        scratch_shapes=[
            pltpu.VMEM((width // LANES, 2, beams, LANES), BF16),
            pltpu.VMEM((width // LANES, 2, beams, LANES), BF16),
            pltpu.VMEM((beams, 2 * LANES), BF16),
            pltpu.VMEM((2, beams, 2 * LANES), BF16),
            pltpu.VMEM((classes, 2 * beams, 2 * LANES), BF16),
            pltpu.SemaphoreType.DMA((2, width // LANES)),
        ],
        input_output_aliases={7: 2},
        compiler_params=pltpu.CompilerParams(vmem_limit_bytes=main_limit(classes)),
        cost_estimate=pl.CostEstimate(
            flops=2 * 20 * beams * beams * width,
            bytes_accessed=beams * beams,
            transcendentals=0,
        ),
        name="main",
    )(own, other, *tables, phase)


def covariance_kernel(scale, *refs):
    parts = (len(refs) - 2) // 2
    kept, received = refs[:parts], refs[parts : 2 * parts]
    spectrum, covariance = refs[2 * parts :]
    classes, rows = kept[0].shape[1:3]
    width = kept[0].shape[3]
    inner = BLOCK // classes
    for h in range(parts):
        spectrum[:, :, :, h * width : (h + 1) * width] = (
            kept[h][...] + received[h][...].astype(F32)
        ) * scale

    def gram(a, b):
        return lax.dot_general(
            a, b, (((1,), (1,)), ((), ())),
            precision=lax.Precision.HIGHEST, preferred_element_type=F32,
        )

    for b in range(rows // inner):
        real, imag = [
            jnp.concatenate(
                [spectrum[t, q, b * inner : (b + 1) * inner, :] for q in range(classes)], axis=0
            )
            for t in range(2)
        ]
        covariance[b] = gram(real, jnp.concatenate([real, -imag], axis=0)) + gram(
            imag, jnp.concatenate([imag, real], axis=0)
        )


def spectrum_and_covariance(kept, received, scale):
    _, classes, rows, width = kept[0].shape
    inner = BLOCK // classes
    return pl.pallas_call(
        functools.partial(covariance_kernel, scale),
        in_specs=[VMEM] * (2 * len(kept)),
        out_specs=[VMEM, VMEM],
        out_shape=[
            jax.ShapeDtypeStruct((2, classes, rows, width * len(kept)), F32),
            jax.ShapeDtypeStruct((rows // inner, BLOCK, 2 * BLOCK), F32),
        ],
        compiler_params=pltpu.CompilerParams(vmem_limit_bytes=SMALL_LIMIT * MIB),
        name="covariance",
    )(*kept, *received)


def focus_kernel(*refs):
    covs, (spectrum, out, stage) = refs[:-3], refs[-3:]
    classes, rows = spectrum.shape[1:3]
    inner = BLOCK // classes
    factor = math.sqrt(BLOCK)
    lane = lax.broadcasted_iota(jnp.int32, (1, 2 * BLOCK), 1)
    first = lane < BLOCK

    def turned(row):
        return pltpu.roll(jnp.broadcast_to(row, (8, 2 * BLOCK)), BLOCK, 1)[0:1]

    for b in range(rows // inner):
        cov = covs[0][b]
        for other in covs[1:]:
            cov = cov + other[b]
        vec_re = jnp.where(first, 1.0, 0.0)
        vec_im = jnp.zeros((1, 2 * BLOCK), F32)
        for step in range(POWER):
            if step % 2 == 0:
                new_re = jnp.sum(
                    cov * jnp.where(first, vec_re, -turned(vec_im)), axis=1, keepdims=True
                )
                new_im = jnp.sum(
                    cov * jnp.where(first, vec_im, turned(vec_re)), axis=1, keepdims=True
                )
                power = jnp.sum(new_re * new_re + new_im * new_im, axis=0, keepdims=True)
            else:
                by_re = jnp.sum(cov * vec_re, axis=0, keepdims=True)
                by_im = jnp.sum(cov * vec_im, axis=0, keepdims=True)
                new_re = jnp.where(first, by_re + turned(by_im), 0.0)
                new_im = jnp.where(first, by_im - turned(by_re), 0.0)
                power = jnp.sum(new_re * new_re + new_im * new_im, axis=1, keepdims=True)
            length = jnp.sqrt(power + EPSILON)
            vec_re = new_re / length
            vec_im = new_im / length
        for q in range(classes):
            re = spectrum[0, q, b * inner : (b + 1) * inner, :]
            im = spectrum[1, q, b * inner : (b + 1) * inner, :]
            by_re = vec_re[q * inner : (q + 1) * inner] * factor
            by_im = vec_im[q * inner : (q + 1) * inner] * factor
            at = pl.ds(q, inner, stride=classes)
            for t, side in enumerate((re * by_re + im * by_im, im * by_re - re * by_im)):
                for j in range(stage.shape[1]):
                    stage[t, j, at, :] = side[:, j * LANES : (j + 1) * LANES]
        for t in range(2):
            for j in range(stage.shape[1]):
                out[t, b * BLOCK : (b + 1) * BLOCK, j * LANES : (j + 1) * LANES] = stage[t, j]


def focus(covs, spectrum):
    _, classes, rows, ranges = spectrum.shape
    return pl.pallas_call(
        focus_kernel,
        in_specs=[VMEM] * (len(covs) + 1),
        out_specs=VMEM,
        out_shape=jax.ShapeDtypeStruct((2, classes * rows, ranges), F32),
        scratch_shapes=[pltpu.VMEM((2, ranges // LANES, BLOCK, LANES), F32)],
        compiler_params=pltpu.CompilerParams(vmem_limit_bytes=SMALL_LIMIT * MIB),
        name="focus",
    )(*covs, spectrum)


def per_device(pulse_data, merge_taps, merge_weights, squint):
    pulses = lax.axis_size("pulse")
    range_count = lax.axis_size("range")
    pulse_index = lax.axis_index("pulse")
    range_index = lax.axis_index("range")
    _, beams, range_cols = pulse_data.shape
    ranges = range_cols * range_count
    angles = beams * pulses
    classes = pulses // 2
    mine, near, far = pack(merge_taps, merge_weights, squint)
    near = swap(near, "pulse", 2)
    middle = swap(far, "pulse", 4)
    far = swap(far, "pulse", 6)
    other = swap(pulse_data, "pulse", 1)
    scalars = jnp.stack(
        [
            pulse_index,
            pulse_index >> 1 & 3,
            (pulse_index & ~6) * beams,
            range_index * range_cols,
        ]
    )
    merge, azimuth = first_tables(scalars, mine, pulses)
    split, join, phase, step = second_tables(scalars, mine, near, middle, far, ranges)
    tables = (merge, split, join, azimuth, step)
    calls = min(CALLS, range_cols // LANES)
    stages = pulses.bit_length() - 1
    halves = [None] * calls

    def advance(part):
        keep, arrived, stage = halves[part]
        total = keep + arrived.astype(F32)
        half = total.shape[2] // 2
        send = total[:, :, half:].astype(BF16)
        arrived = swap(send, "pulse", 1 << stage)
        halves[part] = (total[:, :, :half], arrived, stage + 1)
        return send

    for part in range(calls):
        done = [advance(p) for p in range(part - 1) if halves[p][2] < stages]
        if done:
            phase, done = lax.optimization_barrier((phase, done))
        keep, send, phase = partial_spectrum(part, calls, pulse_data, other, tables, phase, classes)
        halves[part] = (keep, swap(send, "pulse", 1), 1)
    for stage in range(1, stages):
        for part in range(calls):
            if halves[part][2] == stage:
                advance(part)
    kept = [half[0] for half in halves]
    received = [half[1] for half in halves]
    spectrum, cov = spectrum_and_covariance(kept, received, angles ** (-0.5))
    covs = [cov]
    distance = 1
    while distance < range_count:
        total = covs[0]
        for extra in covs[1:]:
            total = total + extra
        covs = [total]
        for turn in range(1, min(4, range_count // distance)):
            covs.append(swap(total, "range", turn * distance))
        distance *= 4
    return focus(covs, spectrum)


def solution(mesh):
    placed = (
        P(None, "pulse", "range"),
        P(None, None, None, "pulse"),
        P(None, None, None, "pulse"),
        P(None, "pulse"),
    )
    return jax.shard_map(
        per_device, mesh=mesh, in_specs=placed, out_specs=P(None, "pulse", "range"), check_vma=False
    )
```

```python
import functools
import math

import jax
import jax.numpy as jnp
from jax import lax
from jax.experimental import pallas as pl
from jax.experimental.pallas import tpu as pltpu
from jax.sharding import PartitionSpec as P


BINS = 1024
BLOCK = 64
POWER = 3
MIB = 1024 * 1024
SMALL_LIMIT = 4
LANES = 128
EPSILON = 1e-06


F32 = jnp.float32
BF16 = jnp.bfloat16


SINE = (3.1415926401307077, -5.16771008350789, 2.550077523214589, -0.5982912856206265, 0.07765766030630428)
COSINE = (0.9999999532476085, -4.934792830619644, 4.058411352862619, -1.3318765680811142, 0.2196896110983216)


def cis_turns(turns):
    z = turns - jnp.floor(turns + 0.5)
    w = z * z
    s, c = SINE[-1], COSINE[-1]
    for more in SINE[-2::-1]:
        s = s * w + more
    for more in COSINE[-2::-1]:
        c = c * w + more
    s = s * z
    twice = s + s
    return 1.0 - twice * s, twice * c


def swap(block, axis, distance):
    count = lax.axis_size(axis)
    return lax.ppermute(block, axis, [(i, i ^ distance) for i in range(count)])


VMEM = pl.BlockSpec(memory_space=pltpu.VMEM)
SMEM = pl.BlockSpec(memory_space=pltpu.SMEM)
HBM = pl.BlockSpec(memory_space=pltpu.HBM)


def pack_kernel(taps, weights, squint, mine, near, far):
    def put(out, row, level, source):
        out[row : row + 4] = taps[level, source].astype(F32)
        out[row + 4 : row + 8] = weights[level, source].astype(F32)

    put(mine, 0, 0, 0)
    put(mine, 8, 0, 1)
    put(mine, 16, 1, 0)
    put(mine, 24, 2, 0)
    mine[32:35] = squint[...]
    mine[35:40] = jnp.zeros((5, mine.shape[1]), F32)
    put(near, 0, 1, 1)
    put(near, 8, 2, 0)
    near[16:19] = squint[...]
    near[19:24] = jnp.zeros((5, near.shape[1]), F32)
    put(far, 0, 2, 1)
    far[8:11] = squint[...]
    far[11:16] = jnp.zeros((5, far.shape[1]), F32)


def pack(taps, weights, squint):
    beams = squint.shape[1]
    return pl.pallas_call(
        pack_kernel,
        in_specs=[VMEM] * 3,
        out_specs=[VMEM] * 3,
        out_shape=[jax.ShapeDtypeStruct((rows, beams), F32) for rows in (40, 24, 16)],
        compiler_params=pltpu.CompilerParams(vmem_limit_bytes=SMALL_LIMIT * MIB),
        name="pack",
    )(taps, weights, squint)


def fill_matrices(columns, outs):
    beams = columns.shape[0]

    def part(i, _):
        at = pl.ds(pl.multiple_of(i * 16, 16), 16)
        lane = lax.broadcasted_iota(jnp.int32, (8, LANES), 1).astype(F32)
        for unit, out in enumerate(outs):
            halves = []
            for h in range(2):
                p = columns[pl.ds(pl.multiple_of(i * 16 + 8 * h, 8), 8), :]
                spread = [
                    jnp.broadcast_to(p[:, 8 * unit + c : 8 * unit + c + 1], (8, LANES))
                    for c in range(8)
                ]
                halves.append(spread)
            for j in range(beams // LANES):
                totals = []
                for spread in halves:
                    total = jnp.zeros((8, LANES), F32)
                    for tap in range(4):
                        total = jnp.where(lane + j * LANES == spread[tap], spread[4 + tap], total)
                    totals.append(total)
                out[at, j * LANES : (j + 1) * LANES] = jnp.concatenate(
                    totals, axis=0
                ).astype(BF16)
        return 0

    lax.fori_loop(0, beams // 16, part, 0, unroll=2)


def first_kernel(pulses, scalars, mine, matrices, table, columns, rows):
    beams = matrices.shape[1]
    angles = beams * pulses
    classes = pulses // 2
    each = BINS // pulses
    rows[0:40] = mine[...]
    columns[...] = rows[...].T
    fill_matrices(columns, [matrices.at[u] for u in range(2)])
    count = BINS // classes
    inner = each // classes
    bits = pulses.bit_length() - 1

    def part(i, _):
        at = pl.ds(pl.multiple_of(i * 16, 16), 16)
        row = lax.broadcasted_iota(jnp.int32, (16, LANES), 0) + i * 16
        group = (row & (count - 1)) >> (inner.bit_length() - 1)
        mirrored = jnp.zeros_like(group)
        for bit in range(bits):
            mirrored = mirrored | ((group >> bit & 1) << (bits - 1 - bit))
        bins = (
            (mirrored ^ scalars[0]) * each
            + (row & (inner - 1)) * classes
            + (row >> (count.bit_length() - 1))
        )
        lane = lax.broadcasted_iota(jnp.int32, (16, LANES), 1)
        whole = angles - 1
        fine_c, fine_s = cis_turns((bins * lane & whole).astype(F32) * (1.0 / angles))
        coarse_c, coarse_s = cis_turns(
            (bins * (scalars[2] + lane * LANES & whole) & whole).astype(F32) * (1.0 / angles)
        )
        low = i * 16 + (i * 16 >> (count.bit_length() - 1)) * count
        cos_at = pl.ds(pl.multiple_of(low, 16), 16)
        sin_at = pl.ds(pl.multiple_of(low + count, 16), 16)
        for j in range(beams // LANES):
            a_c = coarse_c[:, j : j + 1]
            a_s = coarse_s[:, j : j + 1]
            lanes = slice(j * LANES, (j + 1) * LANES)
            table[cos_at, lanes] = (a_c * fine_c - a_s * fine_s).astype(BF16)
            table[sin_at, lanes] = (a_s * fine_c + a_c * fine_s).astype(BF16)
        return 0

    lax.fori_loop(0, BINS // 16, part, 0, unroll=2)


def first_tables(scalars, mine, pulses):
    beams = mine.shape[1]
    return pl.pallas_call(
        functools.partial(first_kernel, pulses),
        in_specs=[SMEM, VMEM],
        out_specs=[VMEM] * 2,
        out_shape=[
            jax.ShapeDtypeStruct((2, beams, beams), BF16),
            jax.ShapeDtypeStruct((2 * BINS, beams), BF16),
        ],
        scratch_shapes=[pltpu.VMEM((beams, LANES), F32), pltpu.VMEM((LANES, beams), F32)],
        compiler_params=pltpu.CompilerParams(vmem_limit_bytes=SMALL_LIMIT * MIB),
        cost_estimate=pl.CostEstimate(
            flops=30 * beams * beams, bytes_accessed=8 * beams * beams, transcendentals=0
        ),
        name="first",
    )(scalars, mine)


def fetch(pulse_data, other, here, there, sems, start):
    return [
        pltpu.make_async_copy(
            source.at[t, :, pl.ds(start + j * LANES, LANES)],
            to.at[j, :, pl.ds(t * LANES, LANES)],
            sems.at[i, j, t],
        )
        for i, (source, to) in enumerate(((pulse_data, here), (other, there)))
        for j in range(here.shape[0])
        for t in range(2)
    ]


def second_kernel(
    ranges,
    scalars, mine, near, middle, far, pulse_data, other,
    split, join, phase, step, here, there,
    columns, rows, packs, sems,
):
    copies = fetch(pulse_data, other, here, there, sems, 0)
    for copy in copies:
        copy.start()
    beams = split.shape[1]
    place = scalars[1]
    packs[0, 0:8] = mine[24:32]
    packs[0, 8:16] = jnp.broadcast_to(mine[34:35], (8, beams))
    packs[1, 0:8] = near[8:16]
    packs[1, 8:16] = jnp.broadcast_to(near[18:19], (8, beams))
    packs[2, 0:8] = middle[0:8]
    packs[2, 8:16] = jnp.broadcast_to(middle[10:11], (8, beams))
    packs[3, 0:8] = far[0:8]
    packs[3, 8:16] = jnp.broadcast_to(far[10:11], (8, beams))
    packs[4, 0:8] = mine[16:24]
    packs[4, 8:16] = jnp.broadcast_to(mine[33:34], (8, beams))
    packs[5, 0:8] = near[0:8]
    packs[5, 8:16] = jnp.broadcast_to(near[17:18], (8, beams))
    order = [4 + (x ^ place & 1) for x in range(2)] + [k ^ place for k in range(4)]
    rows[48:56] = jnp.broadcast_to(mine[32:33], (8, beams))
    for unit, source in enumerate(order):
        rows[8 * unit : 8 * unit + 8] = packs[source, 0:8]
        rows[56 + 8 * unit : 64 + 8 * unit] = packs[source, 8:16]
    columns[...] = rows[...].T
    fill_matrices(
        columns, [split.at[u] for u in range(2)] + [join.at[u] for u in range(4)]
    )

    def part(i, _):
        at = pl.ds(pl.multiple_of(i * 16, 16), 16)
        p = columns[at, :]
        lane = lax.broadcasted_iota(jnp.int32, (16, LANES), 1)
        index = (lane + scalars[3]).astype(F32) * (1.0 / ranges)
        for unit in range(7):
            squint = p[:, 48 + 8 * unit : 49 + 8 * unit]
            cosine, sine = cis_turns(squint * index)
            phase[unit, 0, at, :] = cosine
            phase[unit, 1, at, :] = sine
        cosine, sine = cis_turns(p * (LANES / ranges))
        step[0, at, :] = cosine
        step[1, at, :] = sine
        return 0

    lax.fori_loop(0, beams // 16, part, 0)
    for copy in copies:
        copy.wait()


def second_tables(scalars, mine, near, middle, far, pulse_data, other, ranges, chunks):
    beams = mine.shape[1]
    return pl.pallas_call(
        functools.partial(second_kernel, ranges),
        in_specs=[SMEM] + [VMEM] * 4 + [HBM] * 2,
        out_specs=[VMEM] * 6,
        out_shape=[
            jax.ShapeDtypeStruct((2, beams, beams), BF16),
            jax.ShapeDtypeStruct((4, beams, beams), BF16),
            jax.ShapeDtypeStruct((7, 2, beams, LANES), F32),
            jax.ShapeDtypeStruct((2, beams, LANES), F32),
            jax.ShapeDtypeStruct((chunks, beams, 2 * LANES), BF16),
            jax.ShapeDtypeStruct((chunks, beams, 2 * LANES), BF16),
        ],
        scratch_shapes=[
            pltpu.VMEM((beams, LANES), F32),
            pltpu.VMEM((LANES, beams), F32),
            pltpu.VMEM((6, 16, beams), F32),
            pltpu.SemaphoreType.DMA((2, chunks, 2)),
        ],
        compiler_params=pltpu.CompilerParams(vmem_limit_bytes=SMALL_LIMIT * MIB),
        cost_estimate=pl.CostEstimate(
            flops=60 * beams * beams, bytes_accessed=12 * beams * beams, transcendentals=0
        ),
        name="second",
    )(scalars, mine, near, middle, far, pulse_data, other)


def main_limit(classes):
    return (8 if classes <= 4 else 40) * MIB


def main_kernel(
    start, classes, more,
    near, far, merge, split, join, azimuth, step, phase_in,
    *refs,
):
    if more:
        pulse_data, other, keep, send, phase, here, there, merged, pair, spread, sems = refs
        copies = fetch(pulse_data, other, here, there, sems, start)
    else:
        keep, send, phase, merged, pair, spread = refs
        copies = []
    for copy in copies:
        copy.start()
    beams = merged.shape[0]
    tile = 512
    tiles = beams // tile

    def rotate(unit, at, total):
        cosine = phase[unit, 0, at, :]
        sine = phase[unit, 1, at, :]
        ahead_c = step[0, at, 48 + 8 * unit : 49 + 8 * unit]
        ahead_s = step[1, at, 48 + 8 * unit : 49 + 8 * unit]
        phase[unit, 0, at, :] = cosine * ahead_c - sine * ahead_s
        phase[unit, 1, at, :] = cosine * ahead_s + sine * ahead_c
        real = total[:, :LANES]
        imag = total[:, LANES:]
        return cosine * real - sine * imag, sine * real + cosine * imag

    def product(lhs, rhs):
        return jnp.dot(lhs, rhs, preferred_element_type=F32)

    def chunk(j, _):
        lanes = pl.ds(pl.multiple_of(j * LANES, LANES), LANES)
        for i in range(tiles):
            at = pl.ds(i * tile, tile)
            real, imag = rotate(
                0, at, product(merge[0, at, :], near[j]) + product(merge[1, at, :], far[j])
            )
            merged[at, :LANES] = real.astype(BF16)
            merged[at, LANES:] = imag.astype(BF16)
        for x in range(2):
            for i in range(tiles):
                at = pl.ds(i * tile, tile)
                real, imag = rotate(1 + x, at, product(split[x, at, :], merged[...]))
                pair[x, at, :LANES] = real.astype(BF16)
                pair[x, at, LANES:] = imag.astype(BF16)
        for i in range(tiles):
            at = pl.ds(i * tile, tile)
            terms = [
                rotate(3 + k, at, product(join[k, at, :], pair[k % 2])) for k in range(4)
            ]
            for q in range(classes):
                real = terms[0][0]
                imag = terms[0][1]
                for k in range(1, 4):
                    turn = (q * k) % classes
                    c = math.cos(2.0 * math.pi * turn / classes)
                    s = math.sin(2.0 * math.pi * turn / classes)
                    c = float(round(c)) if abs(c - round(c)) < 1e-9 else c
                    s = float(round(s)) if abs(s - round(s)) < 1e-9 else s
                    re, im = terms[k]
                    for amount, add_re, add_im in ((c, re, im), (s, im, -re)):
                        if amount == 1.0:
                            real, imag = real + add_re, imag + add_im
                        elif amount == -1.0:
                            real, imag = real - add_re, imag - add_im
                        elif amount != 0.0:
                            real, imag = real + amount * add_re, imag + amount * add_im
                spread[q, at, :LANES] = real.astype(BF16)
                spread[q, at, LANES:] = imag.astype(BF16)
        rows = BINS // classes
        half = rows // 2
        for q in range(classes):
            both = product(azimuth[pl.ds(2 * q * rows, 2 * rows), :], spread[q])
            by_cos, by_sin = both[:rows], both[rows:]
            sides = (
                by_cos[:, :LANES] + by_sin[:, LANES:],
                by_cos[:, LANES:] - by_sin[:, :LANES],
            )
            for t, side in enumerate(sides):
                keep[t, q, :, lanes] = side[:half]
                send[t, q, :, lanes] = side[half:].astype(BF16)
        return 0

    lax.fori_loop(0, near.shape[0], chunk, 0)
    for copy in copies:
        copy.wait()


def partial_spectrum(near, far, tables, phase, pulse_data, other, start, chunks, classes):
    beams = near.shape[1]
    width = near.shape[0] * LANES
    half = BINS // classes // 2
    ahead = [jax.ShapeDtypeStruct((chunks, beams, 2 * LANES), BF16)] * 2 if chunks else []
    return pl.pallas_call(
        functools.partial(main_kernel, start, classes, chunks > 0),
        in_specs=[VMEM] * 8 + [HBM] * len(ahead),
        out_specs=[VMEM] * (3 + len(ahead)),
        out_shape=[
            jax.ShapeDtypeStruct((2, classes, half, width), F32),
            jax.ShapeDtypeStruct((2, classes, half, width), BF16),
            jax.ShapeDtypeStruct(phase.shape, F32),
        ]
        + ahead,
        scratch_shapes=[
            pltpu.VMEM((beams, 2 * LANES), BF16),
            pltpu.VMEM((2, beams, 2 * LANES), BF16),
            pltpu.VMEM((classes, beams, 2 * LANES), BF16),
        ]
        + ([pltpu.SemaphoreType.DMA((2, chunks, 2))] if ahead else []),
        input_output_aliases={7: 2},
        compiler_params=pltpu.CompilerParams(vmem_limit_bytes=main_limit(classes)),
        cost_estimate=pl.CostEstimate(
            flops=2 * 20 * beams * beams * width,
            bytes_accessed=beams * beams,
            transcendentals=0,
        ),
        name="main",
    )(near, far, *tables, phase, *([pulse_data, other] if ahead else []))


def covariance_kernel(scale, *refs):
    parts = (len(refs) - 2) // 2
    kept, received = refs[:parts], refs[parts : 2 * parts]
    spectrum, covariance = refs[2 * parts :]
    classes, rows = kept[0].shape[1:3]
    inner = BLOCK // classes
    at = 0
    for h in range(parts):
        width = kept[h].shape[3]
        spectrum[:, :, :, at : at + width] = (
            kept[h][...] + received[h][...].astype(F32)
        ) * scale
        at += width

    def gram(a, b):
        return lax.dot_general(
            a, b, (((1,), (1,)), ((), ())),
            precision=lax.Precision.HIGHEST, preferred_element_type=F32,
        )

    for b in range(rows // inner):
        real, imag = [
            jnp.concatenate(
                [spectrum[t, q, b * inner : (b + 1) * inner, :] for q in range(classes)], axis=0
            )
            for t in range(2)
        ]
        covariance[b] = gram(real, jnp.concatenate([real, -imag], axis=0)) + gram(
            imag, jnp.concatenate([imag, real], axis=0)
        )


def spectrum_and_covariance(kept, received, scale):
    _, classes, rows, _ = kept[0].shape
    width = sum(part.shape[3] for part in kept)
    inner = BLOCK // classes
    return pl.pallas_call(
        functools.partial(covariance_kernel, scale),
        in_specs=[VMEM] * (2 * len(kept)),
        out_specs=[VMEM, VMEM],
        out_shape=[
            jax.ShapeDtypeStruct((2, classes, rows, width), F32),
            jax.ShapeDtypeStruct((rows // inner, BLOCK, 2 * BLOCK), F32),
        ],
        compiler_params=pltpu.CompilerParams(vmem_limit_bytes=SMALL_LIMIT * MIB),
        name="covariance",
    )(*kept, *received)


def focus_kernel(*refs):
    covs, (spectrum, out, stage) = refs[:-3], refs[-3:]
    classes, rows = spectrum.shape[1:3]
    inner = BLOCK // classes
    factor = math.sqrt(BLOCK)
    lane = lax.broadcasted_iota(jnp.int32, (1, 2 * BLOCK), 1)
    first = lane < BLOCK

    def turned(row):
        return pltpu.roll(jnp.broadcast_to(row, (8, 2 * BLOCK)), BLOCK, 1)[0:1]

    for b in range(rows // inner):
        cov = covs[0][b]
        for other in covs[1:]:
            cov = cov + other[b]
        vec_re = jnp.where(first, 1.0, 0.0)
        vec_im = jnp.zeros((1, 2 * BLOCK), F32)
        for step in range(POWER):
            if step % 2 == 0:
                new_re = jnp.sum(
                    cov * jnp.where(first, vec_re, -turned(vec_im)), axis=1, keepdims=True
                )
                new_im = jnp.sum(
                    cov * jnp.where(first, vec_im, turned(vec_re)), axis=1, keepdims=True
                )
                power = jnp.sum(new_re * new_re + new_im * new_im, axis=0, keepdims=True)
            else:
                by_re = jnp.sum(cov * vec_re, axis=0, keepdims=True)
                by_im = jnp.sum(cov * vec_im, axis=0, keepdims=True)
                new_re = jnp.where(first, by_re + turned(by_im), 0.0)
                new_im = jnp.where(first, by_im - turned(by_re), 0.0)
                power = jnp.sum(new_re * new_re + new_im * new_im, axis=1, keepdims=True)
            length = jnp.sqrt(power + EPSILON)
            vec_re = new_re / length
            vec_im = new_im / length
        for q in range(classes):
            re = spectrum[0, q, b * inner : (b + 1) * inner, :]
            im = spectrum[1, q, b * inner : (b + 1) * inner, :]
            by_re = vec_re[q * inner : (q + 1) * inner] * factor
            by_im = vec_im[q * inner : (q + 1) * inner] * factor
            at = pl.ds(q, inner, stride=classes)
            for t, side in enumerate((re * by_re + im * by_im, im * by_re - re * by_im)):
                for j in range(stage.shape[1]):
                    stage[t, j, at, :] = side[:, j * LANES : (j + 1) * LANES]
        for t in range(2):
            for j in range(stage.shape[1]):
                out[t, b * BLOCK : (b + 1) * BLOCK, j * LANES : (j + 1) * LANES] = stage[t, j]


def focus(covs, spectrum):
    _, classes, rows, ranges = spectrum.shape
    return pl.pallas_call(
        focus_kernel,
        in_specs=[VMEM] * (len(covs) + 1),
        out_specs=VMEM,
        out_shape=jax.ShapeDtypeStruct((2, classes * rows, ranges), F32),
        scratch_shapes=[pltpu.VMEM((2, ranges // LANES, BLOCK, LANES), F32)],
        compiler_params=pltpu.CompilerParams(vmem_limit_bytes=SMALL_LIMIT * MIB),
        name="focus",
    )(*covs, spectrum)


def per_device(pulse_data, merge_taps, merge_weights, squint):
    pulses = lax.axis_size("pulse")
    range_count = lax.axis_size("range")
    pulse_index = lax.axis_index("pulse")
    range_index = lax.axis_index("range")
    _, beams, range_cols = pulse_data.shape
    ranges = range_cols * range_count
    angles = beams * pulses
    classes = pulses // 2
    mine, near, far = pack(merge_taps, merge_weights, squint)
    near = swap(near, "pulse", 2)
    middle = swap(far, "pulse", 4)
    far = swap(far, "pulse", 6)
    other = swap(pulse_data, "pulse", 1)
    scalars = jnp.stack(
        [
            pulse_index,
            pulse_index >> 1 & 3,
            (pulse_index & ~6) * beams,
            range_index * range_cols,
        ]
    )
    merge, azimuth = first_tables(scalars, mine, pulses)
    total = range_cols // LANES
    sizes = [2] * (total // 2 - 1) + [1, 1] if total > 2 else [1] * total
    calls = len(sizes)
    split, join, phase, step, here, there = second_tables(
        scalars, mine, near, middle, far, pulse_data, other, ranges, sizes[0]
    )
    tables = (merge, split, join, azimuth, step)
    stages = pulses.bit_length() - 1
    halves = [None] * calls

    def advance(part):
        keep, arrived, stage = halves[part]
        total = keep + arrived.astype(F32)
        half = total.shape[2] // 2
        send = total[:, :, half:].astype(BF16)
        arrived = swap(send, "pulse", 1 << stage)
        halves[part] = (total[:, :, :half], arrived, stage + 1)
        return send

    for part in range(calls):
        done = [advance(p) for p in range(part - 1) if halves[p][2] < stages]
        if done:
            phase, done = lax.optimization_barrier((phase, done))
        keep, send, phase, *ahead = partial_spectrum(
            here, there, tables, phase, pulse_data, other,
            sum(sizes[: part + 1]) * LANES,
            sizes[part + 1] if part + 1 < calls else 0,
            classes,
        )
        if ahead:
            here, there = ahead
        halves[part] = (keep, swap(send, "pulse", 1), 1)
    for stage in range(1, stages):
        for part in range(calls):
            if halves[part][2] == stage:
                advance(part)
    kept = [half[0] for half in halves]
    received = [half[1] for half in halves]
    spectrum, cov = spectrum_and_covariance(kept, received, angles ** (-0.5))
    covs = [cov]
    distance = 1
    while distance < range_count:
        total = covs[0]
        for extra in covs[1:]:
            total = total + extra
        covs = [total]
        for turn in range(1, min(4, range_count // distance)):
            covs.append(swap(total, "range", turn * distance))
        distance *= 4
    return focus(covs, spectrum)


def solution(mesh):
    placed = (
        P(None, "pulse", "range"),
        P(None, None, None, "pulse"),
        P(None, None, None, "pulse"),
        P(None, "pulse"),
    )
    return jax.shard_map(
        per_device, mesh=mesh, in_specs=placed, out_specs=P(None, "pulse", "range"), check_vma=False
    )
```

```python
import functools
import math

import jax
import jax.numpy as jnp
from jax import lax
from jax.experimental import pallas as pl
from jax.experimental.pallas import tpu as pltpu
from jax.sharding import PartitionSpec as P


BINS = 1024
BLOCK = 64
POWER = 3
MIB = 1024 * 1024
SMALL_LIMIT = 4
LANES = 128
EPSILON = 1e-06


F32 = jnp.float32
BF16 = jnp.bfloat16


SINE = (3.1415926401307077, -5.16771008350789, 2.550077523214589, -0.5982912856206265, 0.07765766030630428)
COSINE = (0.9999999532476085, -4.934792830619644, 4.058411352862619, -1.3318765680811142, 0.2196896110983216)


def cis_turns(turns):
    z = turns - jnp.floor(turns + 0.5)
    w = z * z
    s, c = SINE[-1], COSINE[-1]
    for more in SINE[-2::-1]:
        s = s * w + more
    for more in COSINE[-2::-1]:
        c = c * w + more
    s = s * z
    twice = s + s
    return 1.0 - twice * s, twice * c


def swap(block, axis, distance):
    count = lax.axis_size(axis)
    return lax.ppermute(block, axis, [(i, i ^ distance) for i in range(count)])


VMEM = pl.BlockSpec(memory_space=pltpu.VMEM)
SMEM = pl.BlockSpec(memory_space=pltpu.SMEM)
HBM = pl.BlockSpec(memory_space=pltpu.HBM)


def pack_kernel(taps, weights, squint, mine, near, far):
    def put(out, row, level, source):
        out[row : row + 4] = taps[level, source].astype(F32)
        out[row + 4 : row + 8] = weights[level, source].astype(F32)

    put(mine, 0, 0, 0)
    put(mine, 8, 0, 1)
    put(mine, 16, 1, 0)
    put(mine, 24, 2, 0)
    mine[32:35] = squint[...]
    mine[35:40] = jnp.zeros((5, mine.shape[1]), F32)
    put(near, 0, 1, 1)
    put(near, 8, 2, 0)
    near[16:19] = squint[...]
    near[19:24] = jnp.zeros((5, near.shape[1]), F32)
    put(far, 0, 2, 1)
    far[8:11] = squint[...]
    far[11:16] = jnp.zeros((5, far.shape[1]), F32)


def pack(taps, weights, squint):
    beams = squint.shape[1]
    return pl.pallas_call(
        pack_kernel,
        in_specs=[VMEM] * 3,
        out_specs=[VMEM] * 3,
        out_shape=[jax.ShapeDtypeStruct((rows, beams), F32) for rows in (40, 24, 16)],
        compiler_params=pltpu.CompilerParams(vmem_limit_bytes=SMALL_LIMIT * MIB),
        name="pack",
    )(taps, weights, squint)


def fill_matrices(columns, outs):
    beams = columns.shape[0]

    def part(i, _):
        at = pl.ds(pl.multiple_of(i * 16, 16), 16)
        lane = lax.broadcasted_iota(jnp.int32, (16, LANES), 1)
        lanes = [(lane + j * LANES).astype(jnp.int16) for j in range(beams // LANES)]
        p = columns[at, :]

        def spread(column):
            return jnp.broadcast_to(p[:, column : column + 1], (16, LANES))

        for unit, out in enumerate(outs):
            taps = [spread(8 * unit + c).astype(jnp.int32).astype(jnp.int16) for c in range(4)]
            weights = [spread(8 * unit + 4 + c).astype(BF16) for c in range(4)]
            for j, here in enumerate(lanes):
                total = jnp.zeros((16, LANES), BF16)
                for tap, weight in zip(taps, weights):
                    total = jnp.where(here == tap, weight, total)
                out[at, j * LANES : (j + 1) * LANES] = total
        return 0

    lax.fori_loop(0, beams // 16, part, 0, unroll=2)


def first_kernel(pulses, scalars, mine, matrices, table, columns, rows):
    beams = matrices.shape[1]
    angles = beams * pulses
    classes = pulses // 2
    each = BINS // pulses
    rows[0:40] = mine[...]
    columns[...] = rows[...].T
    fill_matrices(columns, [matrices.at[u] for u in range(2)])
    count = BINS // classes
    inner = each // classes
    bits = pulses.bit_length() - 1

    def part(i, _):
        at = pl.ds(pl.multiple_of(i * 16, 16), 16)
        row = lax.broadcasted_iota(jnp.int32, (16, LANES), 0) + i * 16
        group = (row & (count - 1)) >> (inner.bit_length() - 1)
        mirrored = jnp.zeros_like(group)
        for bit in range(bits):
            mirrored = mirrored | ((group >> bit & 1) << (bits - 1 - bit))
        bins = (
            (mirrored ^ scalars[0]) * each
            + (row & (inner - 1)) * classes
            + (row >> (count.bit_length() - 1))
        )
        lane = lax.broadcasted_iota(jnp.int32, (16, LANES), 1)
        whole = angles - 1
        fine_c, fine_s = cis_turns((bins * lane & whole).astype(F32) * (1.0 / angles))
        coarse_c, coarse_s = cis_turns(
            (bins * (scalars[2] + lane * LANES & whole) & whole).astype(F32) * (1.0 / angles)
        )
        low = i * 16 + (i * 16 >> (count.bit_length() - 1)) * count
        cos_at = pl.ds(pl.multiple_of(low, 16), 16)
        sin_at = pl.ds(pl.multiple_of(low + count, 16), 16)
        for j in range(beams // LANES):
            a_c = coarse_c[:, j : j + 1]
            a_s = coarse_s[:, j : j + 1]
            lanes = slice(j * LANES, (j + 1) * LANES)
            table[cos_at, lanes] = (a_c * fine_c - a_s * fine_s).astype(BF16)
            table[sin_at, lanes] = (a_s * fine_c + a_c * fine_s).astype(BF16)
        return 0

    lax.fori_loop(0, BINS // 16, part, 0, unroll=2)


def first_tables(scalars, mine, pulses):
    beams = mine.shape[1]
    return pl.pallas_call(
        functools.partial(first_kernel, pulses),
        in_specs=[SMEM, VMEM],
        out_specs=[VMEM] * 2,
        out_shape=[
            jax.ShapeDtypeStruct((2, beams, beams), BF16),
            jax.ShapeDtypeStruct((2 * BINS, beams), BF16),
        ],
        scratch_shapes=[pltpu.VMEM((beams, LANES), F32), pltpu.VMEM((LANES, beams), F32)],
        compiler_params=pltpu.CompilerParams(vmem_limit_bytes=SMALL_LIMIT * MIB),
        cost_estimate=pl.CostEstimate(
            flops=30 * beams * beams, bytes_accessed=8 * beams * beams, transcendentals=0
        ),
        name="first",
    )(scalars, mine)


def fetch(pulse_data, other, here, there, sems, start):
    return [
        pltpu.make_async_copy(
            source.at[t, :, pl.ds(start + j * LANES, LANES)],
            to.at[j, :, pl.ds(t * LANES, LANES)],
            sems.at[i, j, t],
        )
        for i, (source, to) in enumerate(((pulse_data, here), (other, there)))
        for j in range(here.shape[0])
        for t in range(2)
    ]


def second_kernel(
    ranges,
    scalars, mine, near, middle, far, pulse_data, other,
    split, join, phase, step, here, there,
    columns, rows, packs, sems,
):
    copies = fetch(pulse_data, other, here, there, sems, 0)
    for copy in copies:
        copy.start()
    beams = split.shape[1]
    place = scalars[1]
    packs[0, 0:8] = mine[24:32]
    packs[0, 8:16] = jnp.broadcast_to(mine[34:35], (8, beams))
    packs[1, 0:8] = near[8:16]
    packs[1, 8:16] = jnp.broadcast_to(near[18:19], (8, beams))
    packs[2, 0:8] = middle[0:8]
    packs[2, 8:16] = jnp.broadcast_to(middle[10:11], (8, beams))
    packs[3, 0:8] = far[0:8]
    packs[3, 8:16] = jnp.broadcast_to(far[10:11], (8, beams))
    packs[4, 0:8] = mine[16:24]
    packs[4, 8:16] = jnp.broadcast_to(mine[33:34], (8, beams))
    packs[5, 0:8] = near[0:8]
    packs[5, 8:16] = jnp.broadcast_to(near[17:18], (8, beams))
    order = [4 + (x ^ place & 1) for x in range(2)] + [k ^ place for k in range(4)]
    rows[48:56] = jnp.broadcast_to(mine[32:33], (8, beams))
    for unit, source in enumerate(order):
        rows[8 * unit : 8 * unit + 8] = packs[source, 0:8]
        rows[56 + 8 * unit : 64 + 8 * unit] = packs[source, 8:16]
    columns[...] = rows[...].T
    fill_matrices(
        columns, [split.at[u] for u in range(2)] + [join.at[u] for u in range(4)]
    )

    def part(i, _):
        at = pl.ds(pl.multiple_of(i * 16, 16), 16)
        p = columns[at, :]
        lane = lax.broadcasted_iota(jnp.int32, (16, LANES), 1)
        index = (lane + scalars[3]).astype(F32) * (1.0 / ranges)
        for unit in range(7):
            squint = p[:, 48 + 8 * unit : 49 + 8 * unit]
            cosine, sine = cis_turns(squint * index)
            phase[unit, 0, at, :] = cosine
            phase[unit, 1, at, :] = sine
        cosine, sine = cis_turns(p * (LANES / ranges))
        step[0, at, :] = cosine
        step[1, at, :] = sine
        return 0

    lax.fori_loop(0, beams // 16, part, 0)
    for copy in copies:
        copy.wait()


def second_tables(scalars, mine, near, middle, far, pulse_data, other, ranges, chunks):
    beams = mine.shape[1]
    return pl.pallas_call(
        functools.partial(second_kernel, ranges),
        in_specs=[SMEM] + [VMEM] * 4 + [HBM] * 2,
        out_specs=[VMEM] * 6,
        out_shape=[
            jax.ShapeDtypeStruct((2, beams, beams), BF16),
            jax.ShapeDtypeStruct((4, beams, beams), BF16),
            jax.ShapeDtypeStruct((7, 2, beams, LANES), F32),
            jax.ShapeDtypeStruct((2, beams, LANES), F32),
            jax.ShapeDtypeStruct((chunks, beams, 2 * LANES), BF16),
            jax.ShapeDtypeStruct((chunks, beams, 2 * LANES), BF16),
        ],
        scratch_shapes=[
            pltpu.VMEM((beams, LANES), F32),
            pltpu.VMEM((LANES, beams), F32),
            pltpu.VMEM((6, 16, beams), F32),
            pltpu.SemaphoreType.DMA((2, chunks, 2)),
        ],
        compiler_params=pltpu.CompilerParams(vmem_limit_bytes=SMALL_LIMIT * MIB),
        cost_estimate=pl.CostEstimate(
            flops=60 * beams * beams, bytes_accessed=12 * beams * beams, transcendentals=0
        ),
        name="second",
    )(scalars, mine, near, middle, far, pulse_data, other)


def turned(base, value, turn, count):
    c = math.cos(2.0 * math.pi * turn / count)
    s = math.sin(2.0 * math.pi * turn / count)
    real, imag = base
    re, im = value
    for amount, add_re, add_im in ((c, re, im), (s, im, -re)):
        if abs(amount) < 1e-9:
            continue
        if abs(abs(amount) - 1.0) > 1e-9:
            real, imag = real + amount * add_re, imag + amount * add_im
        elif amount > 0.0:
            real, imag = real + add_re, imag + add_im
        else:
            real, imag = real - add_re, imag - add_im
    return real, imag


def main_limit(classes):
    return (8 if classes <= 4 else 40) * MIB


def main_kernel(
    start, classes, more,
    near, far, merge, split, join, azimuth, step, phase_in,
    *refs,
):
    if more:
        pulse_data, other, keep, send, phase, here, there, merged, pair, spread, sems = refs
        copies = fetch(pulse_data, other, here, there, sems, start)
    else:
        keep, send, phase, merged, pair, spread = refs
        copies = []
    for copy in copies:
        copy.start()
    beams = merged.shape[0]
    tile = 512
    tiles = beams // tile
    small = 256

    def rotate(unit, at, total):
        cosine = phase[unit, 0, at, :]
        sine = phase[unit, 1, at, :]
        ahead_c = step[0, at, 48 + 8 * unit : 49 + 8 * unit]
        ahead_s = step[1, at, 48 + 8 * unit : 49 + 8 * unit]
        phase[unit, 0, at, :] = cosine * ahead_c - sine * ahead_s
        phase[unit, 1, at, :] = cosine * ahead_s + sine * ahead_c
        real = total[:, :LANES]
        imag = total[:, LANES:]
        return cosine * real - sine * imag, sine * real + cosine * imag

    def product(lhs, rhs):
        return jnp.dot(lhs, rhs, preferred_element_type=F32)

    def chunk(j, _):
        lanes = pl.ds(pl.multiple_of(j * LANES, LANES), LANES)
        for i in range(tiles):
            at = pl.ds(i * tile, tile)
            real, imag = rotate(
                0, at, product(merge[0, at, :], near[j]) + product(merge[1, at, :], far[j])
            )
            merged[at, :LANES] = real.astype(BF16)
            merged[at, LANES:] = imag.astype(BF16)
        for x in range(2):
            for i in range(tiles):
                at = pl.ds(i * tile, tile)
                real, imag = rotate(1 + x, at, product(split[x, at, :], merged[...]))
                pair[x, at, :LANES] = real.astype(BF16)
                pair[x, at, LANES:] = imag.astype(BF16)
        for i in range(beams // small):
            at = pl.ds(i * small, small)
            terms = [
                rotate(3 + k, at, product(join[k, at, :], pair[k % 2])) for k in range(4)
            ]
            pairs = {}
            for q in range(classes):
                turn = 2 * q % classes
                if turn not in pairs:
                    pairs[turn] = [turned(terms[x], terms[x + 2], turn, classes) for x in range(2)]
                real, imag = turned(*pairs[turn], q, classes)
                spread[q, at, :LANES] = real.astype(BF16)
                spread[q, at, LANES:] = imag.astype(BF16)
        rows = BINS // classes
        half = rows // 2
        for q in range(classes):
            both = product(azimuth[pl.ds(2 * q * rows, 2 * rows), :], spread[q])
            by_cos, by_sin = both[:rows], both[rows:]
            sides = (
                by_cos[:, :LANES] + by_sin[:, LANES:],
                by_cos[:, LANES:] - by_sin[:, :LANES],
            )
            for t, side in enumerate(sides):
                keep[t, q, :, lanes] = side[:half]
                send[t, q, :, lanes] = side[half:].astype(BF16)
        return 0

    lax.fori_loop(0, near.shape[0], chunk, 0)
    for copy in copies:
        copy.wait()


def partial_spectrum(near, far, tables, phase, pulse_data, other, start, chunks, classes):
    beams = near.shape[1]
    width = near.shape[0] * LANES
    half = BINS // classes // 2
    ahead = [jax.ShapeDtypeStruct((chunks, beams, 2 * LANES), BF16)] * 2 if chunks else []
    return pl.pallas_call(
        functools.partial(main_kernel, start, classes, chunks > 0),
        in_specs=[VMEM] * 8 + [HBM] * len(ahead),
        out_specs=[VMEM] * (3 + len(ahead)),
        out_shape=[
            jax.ShapeDtypeStruct((2, classes, half, width), F32),
            jax.ShapeDtypeStruct((2, classes, half, width), BF16),
            jax.ShapeDtypeStruct(phase.shape, F32),
        ]
        + ahead,
        scratch_shapes=[
            pltpu.VMEM((beams, 2 * LANES), BF16),
            pltpu.VMEM((2, beams, 2 * LANES), BF16),
            pltpu.VMEM((classes, beams, 2 * LANES), BF16),
        ]
        + ([pltpu.SemaphoreType.DMA((2, chunks, 2))] if ahead else []),
        input_output_aliases={7: 2},
        compiler_params=pltpu.CompilerParams(vmem_limit_bytes=main_limit(classes)),
        cost_estimate=pl.CostEstimate(
            flops=2 * 20 * beams * beams * width,
            bytes_accessed=beams * beams,
            transcendentals=0,
        ),
        name="main",
    )(near, far, *tables, phase, *([pulse_data, other] if ahead else []))


def covariance_kernel(scale, *refs):
    parts = (len(refs) - 2) // 2
    kept, received = refs[:parts], refs[parts : 2 * parts]
    spectrum, covariance = refs[2 * parts :]
    classes, rows = kept[0].shape[1:3]
    inner = BLOCK // classes
    at = 0
    for h in range(parts):
        width = kept[h].shape[3]
        spectrum[:, :, :, at : at + width] = (
            kept[h][...] + received[h][...].astype(F32)
        ) * scale
        at += width

    def gram(a, b):
        return lax.dot_general(
            a, b, (((1,), (1,)), ((), ())),
            precision=lax.Precision.HIGHEST, preferred_element_type=F32,
        )

    def block(b, _):
        at = pl.ds(pl.multiple_of(b * inner, inner), inner)
        real, imag = [
            jnp.concatenate([spectrum[t, q, at, :] for q in range(classes)], axis=0)
            for t in range(2)
        ]
        covariance[b] = gram(real, jnp.concatenate([real, -imag], axis=0)) + gram(
            imag, jnp.concatenate([imag, real], axis=0)
        )
        return 0

    lax.fori_loop(0, rows // inner, block, 0)


def spectrum_and_covariance(kept, received, scale):
    _, classes, rows, _ = kept[0].shape
    width = sum(part.shape[3] for part in kept)
    inner = BLOCK // classes
    return pl.pallas_call(
        functools.partial(covariance_kernel, scale),
        in_specs=[VMEM] * (2 * len(kept)),
        out_specs=[VMEM, VMEM],
        out_shape=[
            jax.ShapeDtypeStruct((2, classes, rows, width), F32),
            jax.ShapeDtypeStruct((rows // inner, BLOCK, 2 * BLOCK), F32),
        ],
        compiler_params=pltpu.CompilerParams(vmem_limit_bytes=SMALL_LIMIT * MIB),
        name="covariance",
    )(*kept, *received)


def focus_kernel(*refs):
    covs, (spectrum, out, stage) = refs[:-3], refs[-3:]
    classes, rows = spectrum.shape[1:3]
    inner = BLOCK // classes
    factor = math.sqrt(BLOCK)
    lane = lax.broadcasted_iota(jnp.int32, (1, 2 * BLOCK), 1)
    first = lane < BLOCK

    def turned(row):
        return pltpu.roll(jnp.broadcast_to(row, (8, 2 * BLOCK)), BLOCK, 1)[0:1]

    for b in range(rows // inner):
        cov = covs[0][b]
        for other in covs[1:]:
            cov = cov + other[b]
        vec_re = jnp.where(first, 1.0, 0.0)
        vec_im = jnp.zeros((1, 2 * BLOCK), F32)
        for step in range(POWER):
            if step % 2 == 0:
                new_re = jnp.sum(
                    cov * jnp.where(first, vec_re, -turned(vec_im)), axis=1, keepdims=True
                )
                new_im = jnp.sum(
                    cov * jnp.where(first, vec_im, turned(vec_re)), axis=1, keepdims=True
                )
                power = jnp.sum(new_re * new_re + new_im * new_im, axis=0, keepdims=True)
            else:
                by_re = jnp.sum(cov * vec_re, axis=0, keepdims=True)
                by_im = jnp.sum(cov * vec_im, axis=0, keepdims=True)
                new_re = jnp.where(first, by_re + turned(by_im), 0.0)
                new_im = jnp.where(first, by_im - turned(by_re), 0.0)
                power = jnp.sum(new_re * new_re + new_im * new_im, axis=1, keepdims=True)
            length = jnp.sqrt(power + EPSILON)
            vec_re = new_re / length
            vec_im = new_im / length
        for q in range(classes):
            re = spectrum[0, q, b * inner : (b + 1) * inner, :]
            im = spectrum[1, q, b * inner : (b + 1) * inner, :]
            by_re = vec_re[q * inner : (q + 1) * inner] * factor
            by_im = vec_im[q * inner : (q + 1) * inner] * factor
            at = pl.ds(q, inner, stride=classes)
            for t, side in enumerate((re * by_re + im * by_im, im * by_re - re * by_im)):
                for j in range(stage.shape[1]):
                    stage[t, j, at, :] = side[:, j * LANES : (j + 1) * LANES]
        for t in range(2):
            for j in range(stage.shape[1]):
                out[t, b * BLOCK : (b + 1) * BLOCK, j * LANES : (j + 1) * LANES] = stage[t, j]


def focus(covs, spectrum):
    _, classes, rows, ranges = spectrum.shape
    return pl.pallas_call(
        focus_kernel,
        in_specs=[VMEM] * (len(covs) + 1),
        out_specs=VMEM,
        out_shape=jax.ShapeDtypeStruct((2, classes * rows, ranges), F32),
        scratch_shapes=[pltpu.VMEM((2, ranges // LANES, BLOCK, LANES), F32)],
        compiler_params=pltpu.CompilerParams(vmem_limit_bytes=SMALL_LIMIT * MIB),
        name="focus",
    )(*covs, spectrum)


def per_device(pulse_data, merge_taps, merge_weights, squint):
    pulses = lax.axis_size("pulse")
    range_count = lax.axis_size("range")
    pulse_index = lax.axis_index("pulse")
    range_index = lax.axis_index("range")
    _, beams, range_cols = pulse_data.shape
    ranges = range_cols * range_count
    angles = beams * pulses
    classes = pulses // 2
    mine, near, far = pack(merge_taps, merge_weights, squint)
    near = swap(near, "pulse", 2)
    middle = swap(far, "pulse", 4)
    far = swap(far, "pulse", 6)
    other = swap(pulse_data, "pulse", 1)
    scalars = jnp.stack(
        [
            pulse_index,
            pulse_index >> 1 & 3,
            (pulse_index & ~6) * beams,
            range_index * range_cols,
        ]
    )
    merge, azimuth = first_tables(scalars, mine, pulses)
    total = range_cols // LANES
    sizes = [total // 4, total // 4, total // 4, total - total // 8 * 7, total // 8] if total >= 8 else [1] * total
    calls = len(sizes)
    split, join, phase, step, here, there = second_tables(
        scalars, mine, near, middle, far, pulse_data, other, ranges, sizes[0]
    )
    tables = (merge, split, join, azimuth, step)
    stages = pulses.bit_length() - 1
    halves = [None] * calls

    def advance(part):
        keep, arrived, stage = halves[part]
        total = keep + arrived.astype(F32)
        half = total.shape[2] // 2
        send = total[:, :, half:].astype(BF16)
        arrived = swap(send, "pulse", 1 << stage)
        halves[part] = (total[:, :, :half], arrived, stage + 1)
        return send

    for part in range(calls):
        done = [advance(p) for p in range(part - 1) if halves[p][2] < stages]
        if done:
            phase, done = lax.optimization_barrier((phase, done))
        keep, send, phase, *ahead = partial_spectrum(
            here, there, tables, phase, pulse_data, other,
            sum(sizes[: part + 1]) * LANES,
            sizes[part + 1] if part + 1 < calls else 0,
            classes,
        )
        if ahead:
            here, there = ahead
        halves[part] = (keep, swap(send, "pulse", 1), 1)
    for stage in range(1, stages):
        for part in range(calls):
            if halves[part][2] == stage:
                advance(part)
    kept = [half[0] for half in halves]
    received = [half[1] for half in halves]
    spectrum, cov = spectrum_and_covariance(kept, received, angles ** (-0.5))
    covs = [cov]
    distance = 1
    while distance < range_count:
        total = covs[0]
        for extra in covs[1:]:
            total = total + extra
        covs = [total]
        for turn in range(1, min(4, range_count // distance)):
            covs.append(swap(total, "range", turn * distance))
        distance *= 4
    return focus(covs, spectrum)


def solution(mesh):
    placed = (
        P(None, "pulse", "range"),
        P(None, None, None, "pulse"),
        P(None, None, None, "pulse"),
        P(None, "pulse"),
    )
    return jax.shard_map(
        per_device, mesh=mesh, in_specs=placed, out_specs=P(None, "pulse", "range"), check_vma=False
    )
```

```python
import functools
import math

import jax
import jax.numpy as jnp
from jax import lax
from jax.experimental import pallas as pl
from jax.experimental.pallas import tpu as pltpu
from jax.sharding import PartitionSpec as P


BINS = 1024
BLOCK = 64
POWER = 3
MIB = 1024 * 1024
SMALL_LIMIT = 4
LANES = 128
EPSILON = 1e-06


F32 = jnp.float32
BF16 = jnp.bfloat16


SINE = (3.1415926401307077, -5.16771008350789, 2.550077523214589, -0.5982912856206265, 0.07765766030630428)
COSINE = (0.9999999532476085, -4.934792830619644, 4.058411352862619, -1.3318765680811142, 0.2196896110983216)


def cis_turns(turns):
    z = turns - jnp.floor(turns + 0.5)
    w = z * z
    s, c = SINE[-1], COSINE[-1]
    for more in SINE[-2::-1]:
        s = s * w + more
    for more in COSINE[-2::-1]:
        c = c * w + more
    s = s * z
    twice = s + s
    return 1.0 - twice * s, twice * c


def swap(block, axis, distance):
    count = lax.axis_size(axis)
    return lax.ppermute(block, axis, [(i, i ^ distance) for i in range(count)])


VMEM = pl.BlockSpec(memory_space=pltpu.VMEM)
SMEM = pl.BlockSpec(memory_space=pltpu.SMEM)
HBM = pl.BlockSpec(memory_space=pltpu.HBM)


def pack_kernel(taps, weights, squint, mine, near, far):
    def put(out, row, level, source):
        out[row : row + 4] = taps[level, source].astype(F32)
        out[row + 4 : row + 8] = weights[level, source].astype(F32)

    put(mine, 0, 0, 0)
    put(mine, 8, 0, 1)
    put(mine, 16, 1, 0)
    put(mine, 24, 2, 0)
    mine[32:35] = squint[...]
    mine[35:40] = jnp.zeros((5, mine.shape[1]), F32)
    put(near, 0, 1, 1)
    put(near, 8, 2, 0)
    near[16:19] = squint[...]
    near[19:24] = jnp.zeros((5, near.shape[1]), F32)
    put(far, 0, 2, 1)
    far[8:11] = squint[...]
    far[11:16] = jnp.zeros((5, far.shape[1]), F32)


def pack(taps, weights, squint):
    beams = squint.shape[1]
    return pl.pallas_call(
        pack_kernel,
        in_specs=[VMEM] * 3,
        out_specs=[VMEM] * 3,
        out_shape=[jax.ShapeDtypeStruct((rows, beams), F32) for rows in (40, 24, 16)],
        compiler_params=pltpu.CompilerParams(vmem_limit_bytes=SMALL_LIMIT * MIB),
        name="pack",
    )(taps, weights, squint)


def fill_matrices(columns, outs):
    beams = columns.shape[0]

    def part(i, _):
        at = pl.ds(pl.multiple_of(i * 16, 16), 16)
        lane = lax.broadcasted_iota(jnp.int32, (16, LANES), 1)
        lanes = [(lane + j * LANES).astype(jnp.int16) for j in range(beams // LANES)]
        whole = columns[at, :].astype(jnp.int32).astype(jnp.int16)
        real = columns[at, :].astype(BF16)

        def spread(value, column):
            return jnp.broadcast_to(value[:, column : column + 1], (16, LANES))

        for unit, out in enumerate(outs):
            taps = [spread(whole, 8 * unit + c) for c in range(4)]
            weights = [spread(real, 8 * unit + 4 + c) for c in range(4)]
            for j, here in enumerate(lanes):
                total = jnp.zeros((16, LANES), BF16)
                for tap, weight in zip(taps, weights):
                    total = jnp.where(here == tap, weight, total)
                out[at, j * LANES : (j + 1) * LANES] = total
        return 0

    lax.fori_loop(0, beams // 16, part, 0, unroll=2)


def first_kernel(pulses, scalars, mine, matrices, table, columns, rows):
    beams = matrices.shape[1]
    angles = beams * pulses
    classes = pulses // 2
    each = BINS // pulses
    rows[0:40] = mine[...]
    columns[...] = rows[...].T
    fill_matrices(columns, [matrices.at[u] for u in range(2)])
    count = BINS // classes
    inner = each // classes
    bits = pulses.bit_length() - 1

    def part(i, _):
        at = pl.ds(pl.multiple_of(i * 16, 16), 16)
        row = lax.broadcasted_iota(jnp.int32, (16, LANES), 0) + i * 16
        group = (row & (count - 1)) >> (inner.bit_length() - 1)
        mirrored = jnp.zeros_like(group)
        for bit in range(bits):
            mirrored = mirrored | ((group >> bit & 1) << (bits - 1 - bit))
        bins = (
            (mirrored ^ scalars[0]) * each
            + (row & (inner - 1)) * classes
            + (row >> (count.bit_length() - 1))
        )
        lane = lax.broadcasted_iota(jnp.int32, (16, LANES), 1)
        whole = angles - 1
        cosine, sine = cis_turns(
            (bins * (scalars[2] + lane & whole) & whole).astype(F32) * (1.0 / angles)
        )
        ahead_c, ahead_s = cis_turns((bins * LANES & whole).astype(F32) * (1.0 / angles))
        low = i * 16 + (i * 16 >> (count.bit_length() - 1)) * count
        cos_at = pl.ds(pl.multiple_of(low, 16), 16)
        sin_at = pl.ds(pl.multiple_of(low + count, 16), 16)
        for j in range(beams // LANES):
            lanes = slice(j * LANES, (j + 1) * LANES)
            table[cos_at, lanes] = cosine.astype(BF16)
            table[sin_at, lanes] = sine.astype(BF16)
            cosine, sine = (
                cosine * ahead_c - sine * ahead_s,
                sine * ahead_c + cosine * ahead_s,
            )
        return 0

    lax.fori_loop(0, BINS // 16, part, 0, unroll=2)


def first_tables(scalars, mine, pulses):
    beams = mine.shape[1]
    return pl.pallas_call(
        functools.partial(first_kernel, pulses),
        in_specs=[SMEM, VMEM],
        out_specs=[VMEM] * 2,
        out_shape=[
            jax.ShapeDtypeStruct((2, beams, beams), BF16),
            jax.ShapeDtypeStruct((2 * BINS, beams), BF16),
        ],
        scratch_shapes=[pltpu.VMEM((beams, LANES), F32), pltpu.VMEM((LANES, beams), F32)],
        compiler_params=pltpu.CompilerParams(vmem_limit_bytes=SMALL_LIMIT * MIB),
        cost_estimate=pl.CostEstimate(
            flops=30 * beams * beams, bytes_accessed=8 * beams * beams, transcendentals=0
        ),
        name="first",
    )(scalars, mine)


def fetch(pulse_data, other, here, there, sems, start):
    return [
        pltpu.make_async_copy(
            source.at[t, :, pl.ds(start + j * LANES, LANES)],
            to.at[j, :, pl.ds(t * LANES, LANES)],
            sems.at[i, j, t],
        )
        for i, (source, to) in enumerate(((pulse_data, here), (other, there)))
        for j in range(here.shape[0])
        for t in range(2)
    ]


def second_kernel(
    ranges,
    scalars, mine, near, middle, far, pulse_data, other,
    split, join, phase, step, here, there,
    columns, rows, packs, sems,
):
    copies = fetch(pulse_data, other, here, there, sems, 0)
    for copy in copies:
        copy.start()
    beams = split.shape[1]
    place = scalars[1]
    packs[0, 0:8] = mine[24:32]
    packs[0, 8:16] = jnp.broadcast_to(mine[34:35], (8, beams))
    packs[1, 0:8] = near[8:16]
    packs[1, 8:16] = jnp.broadcast_to(near[18:19], (8, beams))
    packs[2, 0:8] = middle[0:8]
    packs[2, 8:16] = jnp.broadcast_to(middle[10:11], (8, beams))
    packs[3, 0:8] = far[0:8]
    packs[3, 8:16] = jnp.broadcast_to(far[10:11], (8, beams))
    packs[4, 0:8] = mine[16:24]
    packs[4, 8:16] = jnp.broadcast_to(mine[33:34], (8, beams))
    packs[5, 0:8] = near[0:8]
    packs[5, 8:16] = jnp.broadcast_to(near[17:18], (8, beams))
    order = [4 + (x ^ place & 1) for x in range(2)] + [k ^ place for k in range(4)]
    rows[48:56] = jnp.broadcast_to(mine[32:33], (8, beams))
    for unit, source in enumerate(order):
        rows[8 * unit : 8 * unit + 8] = packs[source, 0:8]
        rows[56 + 8 * unit : 64 + 8 * unit] = packs[source, 8:16]
    columns[...] = rows[...].T
    fill_matrices(
        columns, [split.at[u] for u in range(2)] + [join.at[u] for u in range(4)]
    )

    def part(i, _):
        at = pl.ds(pl.multiple_of(i * 16, 16), 16)
        p = columns[at, :]
        lane = lax.broadcasted_iota(jnp.int32, (16, LANES), 1)
        index = (lane + scalars[3]).astype(F32) * (1.0 / ranges)
        for unit in range(7):
            squint = p[:, 48 + 8 * unit : 49 + 8 * unit]
            cosine, sine = cis_turns(squint * index)
            phase[unit, 0, at, :] = cosine
            phase[unit, 1, at, :] = sine
        cosine, sine = cis_turns(p * (LANES / ranges))
        step[0, at, :] = cosine
        step[1, at, :] = sine
        return 0

    lax.fori_loop(0, beams // 16, part, 0)
    for copy in copies:
        copy.wait()


def second_tables(scalars, mine, near, middle, far, pulse_data, other, ranges, chunks):
    beams = mine.shape[1]
    return pl.pallas_call(
        functools.partial(second_kernel, ranges),
        in_specs=[SMEM] + [VMEM] * 4 + [HBM] * 2,
        out_specs=[VMEM] * 6,
        out_shape=[
            jax.ShapeDtypeStruct((2, beams, beams), BF16),
            jax.ShapeDtypeStruct((4, beams, beams), BF16),
            jax.ShapeDtypeStruct((7, 2, beams, LANES), F32),
            jax.ShapeDtypeStruct((2, beams, LANES), F32),
            jax.ShapeDtypeStruct((chunks, beams, 2 * LANES), BF16),
            jax.ShapeDtypeStruct((chunks, beams, 2 * LANES), BF16),
        ],
        scratch_shapes=[
            pltpu.VMEM((beams, LANES), F32),
            pltpu.VMEM((LANES, beams), F32),
            pltpu.VMEM((6, 16, beams), F32),
            pltpu.SemaphoreType.DMA((2, chunks, 2)),
        ],
        compiler_params=pltpu.CompilerParams(vmem_limit_bytes=SMALL_LIMIT * MIB),
        cost_estimate=pl.CostEstimate(
            flops=60 * beams * beams, bytes_accessed=12 * beams * beams, transcendentals=0
        ),
        name="second",
    )(scalars, mine, near, middle, far, pulse_data, other)


def turned(base, value, turn, count):
    c = math.cos(2.0 * math.pi * turn / count)
    s = math.sin(2.0 * math.pi * turn / count)
    real, imag = base
    re, im = value
    for amount, add_re, add_im in ((c, re, im), (s, im, -re)):
        if abs(amount) < 1e-9:
            continue
        if abs(abs(amount) - 1.0) > 1e-9:
            real, imag = real + amount * add_re, imag + amount * add_im
        elif amount > 0.0:
            real, imag = real + add_re, imag + add_im
        else:
            real, imag = real - add_re, imag - add_im
    return real, imag


def main_limit(classes):
    return (8 if classes <= 4 else 40) * MIB


def main_kernel(
    start, classes, more,
    near, far, merge, split, join, azimuth, step, phase_in,
    *refs,
):
    if more:
        pulse_data, other, keep, send, phase, here, there, merged, pair, spread, sems = refs
        copies = fetch(pulse_data, other, here, there, sems, start)
    else:
        keep, send, phase, merged, pair, spread = refs
        copies = []
    for copy in copies:
        copy.start()
    beams = merged.shape[0]
    tile = 512
    tiles = beams // tile
    small = 256

    def rotate(unit, at, total):
        cosine = phase[unit, 0, at, :]
        sine = phase[unit, 1, at, :]
        ahead_c = step[0, at, 48 + 8 * unit : 49 + 8 * unit]
        ahead_s = step[1, at, 48 + 8 * unit : 49 + 8 * unit]
        phase[unit, 0, at, :] = cosine * ahead_c - sine * ahead_s
        phase[unit, 1, at, :] = cosine * ahead_s + sine * ahead_c
        real = total[:, :LANES]
        imag = total[:, LANES:]
        return cosine * real - sine * imag, sine * real + cosine * imag

    def product(lhs, rhs):
        return jnp.dot(lhs, rhs, preferred_element_type=F32)

    def chunk(j, _):
        lanes = pl.ds(pl.multiple_of(j * LANES, LANES), LANES)
        for i in range(tiles):
            at = pl.ds(i * tile, tile)
            real, imag = rotate(
                0, at, product(merge[0, at, :], near[j]) + product(merge[1, at, :], far[j])
            )
            merged[at, :LANES] = real.astype(BF16)
            merged[at, LANES:] = imag.astype(BF16)
        for x in range(2):
            for i in range(tiles):
                at = pl.ds(i * tile, tile)
                real, imag = rotate(1 + x, at, product(split[x, at, :], merged[...]))
                pair[x, at, :LANES] = real.astype(BF16)
                pair[x, at, LANES:] = imag.astype(BF16)
        for i in range(beams // small):
            at = pl.ds(i * small, small)
            terms = [
                rotate(3 + k, at, product(join[k, at, :], pair[k % 2])) for k in range(4)
            ]
            pairs = {}
            for q in range(classes):
                turn = 2 * q % classes
                if turn not in pairs:
                    pairs[turn] = [turned(terms[x], terms[x + 2], turn, classes) for x in range(2)]
                real, imag = turned(*pairs[turn], q, classes)
                spread[q, at, :LANES] = real.astype(BF16)
                spread[q, at, LANES:] = imag.astype(BF16)
        rows = BINS // classes
        half = rows // 2
        for q in range(classes):
            both = product(azimuth[pl.ds(2 * q * rows, 2 * rows), :], spread[q])
            by_cos, by_sin = both[:rows], both[rows:]
            sides = (
                by_cos[:, :LANES] + by_sin[:, LANES:],
                by_cos[:, LANES:] - by_sin[:, :LANES],
            )
            for t, side in enumerate(sides):
                keep[t, q, :, lanes] = side[:half]
                send[t, q, :, lanes] = side[half:].astype(BF16)
        return 0

    lax.fori_loop(0, near.shape[0], chunk, 0)
    for copy in copies:
        copy.wait()


def partial_spectrum(near, far, tables, phase, pulse_data, other, start, chunks, classes):
    beams = near.shape[1]
    width = near.shape[0] * LANES
    half = BINS // classes // 2
    ahead = [jax.ShapeDtypeStruct((chunks, beams, 2 * LANES), BF16)] * 2 if chunks else []
    return pl.pallas_call(
        functools.partial(main_kernel, start, classes, chunks > 0),
        in_specs=[VMEM] * 8 + [HBM] * len(ahead),
        out_specs=[VMEM] * (3 + len(ahead)),
        out_shape=[
            jax.ShapeDtypeStruct((2, classes, half, width), F32),
            jax.ShapeDtypeStruct((2, classes, half, width), BF16),
            jax.ShapeDtypeStruct(phase.shape, F32),
        ]
        + ahead,
        scratch_shapes=[
            pltpu.VMEM((beams, 2 * LANES), BF16),
            pltpu.VMEM((2, beams, 2 * LANES), BF16),
            pltpu.VMEM((classes, beams, 2 * LANES), BF16),
        ]
        + ([pltpu.SemaphoreType.DMA((2, chunks, 2))] if ahead else []),
        input_output_aliases={7: 2},
        compiler_params=pltpu.CompilerParams(vmem_limit_bytes=main_limit(classes)),
        cost_estimate=pl.CostEstimate(
            flops=2 * 20 * beams * beams * width,
            bytes_accessed=beams * beams,
            transcendentals=0,
        ),
        name="main",
    )(near, far, *tables, phase, *([pulse_data, other] if ahead else []))


def covariance_kernel(scale, *refs):
    parts = (len(refs) - 2) // 2
    kept, received = refs[:parts], refs[parts : 2 * parts]
    spectrum, covariance = refs[2 * parts :]
    classes, rows = kept[0].shape[1:3]
    inner = BLOCK // classes
    at = 0
    for h in range(parts):
        width = kept[h].shape[3]
        spectrum[:, :, :, at : at + width] = (
            kept[h][...] + received[h][...].astype(F32)
        ) * scale
        at += width

    def gram(a, b):
        return lax.dot_general(
            a, b, (((1,), (1,)), ((), ())),
            precision=lax.Precision.HIGHEST, preferred_element_type=F32,
        )

    def block(b, _):
        at = pl.ds(pl.multiple_of(b * inner, inner), inner)
        real, imag = [
            jnp.concatenate([spectrum[t, q, at, :] for q in range(classes)], axis=0)
            for t in range(2)
        ]
        covariance[b] = gram(real, jnp.concatenate([real, -imag], axis=0)) + gram(
            imag, jnp.concatenate([imag, real], axis=0)
        )
        return 0

    lax.fori_loop(0, rows // inner, block, 0)


def spectrum_and_covariance(kept, received, scale):
    _, classes, rows, _ = kept[0].shape
    width = sum(part.shape[3] for part in kept)
    inner = BLOCK // classes
    return pl.pallas_call(
        functools.partial(covariance_kernel, scale),
        in_specs=[VMEM] * (2 * len(kept)),
        out_specs=[VMEM, VMEM],
        out_shape=[
            jax.ShapeDtypeStruct((2, classes, rows, width), F32),
            jax.ShapeDtypeStruct((rows // inner, BLOCK, 2 * BLOCK), F32),
        ],
        compiler_params=pltpu.CompilerParams(vmem_limit_bytes=SMALL_LIMIT * MIB),
        name="covariance",
    )(*kept, *received)


def focus_kernel(*refs):
    covs, (spectrum, out, stage) = refs[:-3], refs[-3:]
    classes, rows = spectrum.shape[1:3]
    inner = BLOCK // classes
    factor = math.sqrt(BLOCK)
    lane = lax.broadcasted_iota(jnp.int32, (1, 2 * BLOCK), 1)
    first = lane < BLOCK

    def turned(row):
        return pltpu.roll(jnp.broadcast_to(row, (8, 2 * BLOCK)), BLOCK, 1)[0:1]

    for b in range(rows // inner):
        cov = covs[0][b]
        for other in covs[1:]:
            cov = cov + other[b]
        vec_re = jnp.where(first, 1.0, 0.0)
        vec_im = jnp.zeros((1, 2 * BLOCK), F32)
        for step in range(POWER):
            if step % 2 == 0:
                new_re = jnp.sum(
                    cov * jnp.where(first, vec_re, -turned(vec_im)), axis=1, keepdims=True
                )
                new_im = jnp.sum(
                    cov * jnp.where(first, vec_im, turned(vec_re)), axis=1, keepdims=True
                )
                power = jnp.sum(new_re * new_re + new_im * new_im, axis=0, keepdims=True)
            else:
                by_re = jnp.sum(cov * vec_re, axis=0, keepdims=True)
                by_im = jnp.sum(cov * vec_im, axis=0, keepdims=True)
                new_re = jnp.where(first, by_re + turned(by_im), 0.0)
                new_im = jnp.where(first, by_im - turned(by_re), 0.0)
                power = jnp.sum(new_re * new_re + new_im * new_im, axis=1, keepdims=True)
            length = jnp.sqrt(power + EPSILON)
            vec_re = new_re / length
            vec_im = new_im / length
        for q in range(classes):
            re = spectrum[0, q, b * inner : (b + 1) * inner, :]
            im = spectrum[1, q, b * inner : (b + 1) * inner, :]
            by_re = vec_re[q * inner : (q + 1) * inner] * factor
            by_im = vec_im[q * inner : (q + 1) * inner] * factor
            at = pl.ds(q, inner, stride=classes)
            for t, side in enumerate((re * by_re + im * by_im, im * by_re - re * by_im)):
                for j in range(stage.shape[1]):
                    stage[t, j, at, :] = side[:, j * LANES : (j + 1) * LANES]
        for t in range(2):
            for j in range(stage.shape[1]):
                out[t, b * BLOCK : (b + 1) * BLOCK, j * LANES : (j + 1) * LANES] = stage[t, j]


def focus(covs, spectrum):
    _, classes, rows, ranges = spectrum.shape
    return pl.pallas_call(
        focus_kernel,
        in_specs=[VMEM] * (len(covs) + 1),
        out_specs=VMEM,
        out_shape=jax.ShapeDtypeStruct((2, classes * rows, ranges), F32),
        scratch_shapes=[pltpu.VMEM((2, ranges // LANES, BLOCK, LANES), F32)],
        compiler_params=pltpu.CompilerParams(vmem_limit_bytes=SMALL_LIMIT * MIB),
        name="focus",
    )(*covs, spectrum)


def per_device(pulse_data, merge_taps, merge_weights, squint):
    pulses = lax.axis_size("pulse")
    range_count = lax.axis_size("range")
    pulse_index = lax.axis_index("pulse")
    range_index = lax.axis_index("range")
    _, beams, range_cols = pulse_data.shape
    ranges = range_cols * range_count
    angles = beams * pulses
    classes = pulses // 2
    mine, near, far = pack(merge_taps, merge_weights, squint)
    near = swap(near, "pulse", 2)
    middle = swap(far, "pulse", 4)
    far = swap(far, "pulse", 6)
    other = swap(pulse_data, "pulse", 1)
    scalars = jnp.stack(
        [
            pulse_index,
            pulse_index >> 1 & 3,
            (pulse_index & ~6) * beams,
            range_index * range_cols,
        ]
    )
    merge, azimuth = first_tables(scalars, mine, pulses)
    total = range_cols // LANES
    sizes = [total // 4, total // 4, total // 4, total - total // 8 * 7, total // 8] if total >= 8 else [1] * total
    calls = len(sizes)
    split, join, phase, step, here, there = second_tables(
        scalars, mine, near, middle, far, pulse_data, other, ranges, sizes[0]
    )
    tables = (merge, split, join, azimuth, step)
    stages = pulses.bit_length() - 1
    halves = [None] * calls

    def advance(part):
        keep, arrived, stage = halves[part]
        total = keep + arrived.astype(F32)
        half = total.shape[2] // 2
        send = total[:, :, half:].astype(BF16)
        arrived = swap(send, "pulse", 1 << stage)
        halves[part] = (total[:, :, :half], arrived, stage + 1)
        return send

    for part in range(calls):
        done = [advance(p) for p in range(part - 1) if halves[p][2] < stages]
        if done:
            phase, done = lax.optimization_barrier((phase, done))
        keep, send, phase, *ahead = partial_spectrum(
            here, there, tables, phase, pulse_data, other,
            sum(sizes[: part + 1]) * LANES,
            sizes[part + 1] if part + 1 < calls else 0,
            classes,
        )
        if ahead:
            here, there = ahead
        halves[part] = (keep, swap(send, "pulse", 1), 1)
    for stage in range(1, stages):
        for part in range(calls):
            if halves[part][2] == stage:
                advance(part)
    kept = [half[0] for half in halves]
    received = [half[1] for half in halves]
    spectrum, cov = spectrum_and_covariance(kept, received, angles ** (-0.5))
    covs = [cov]
    distance = 1
    while distance < range_count:
        total = covs[0]
        for extra in covs[1:]:
            total = total + extra
        covs = [total]
        for turn in range(1, min(4, range_count // distance)):
            covs.append(swap(total, "range", turn * distance))
        distance *= 4
    return focus(covs, spectrum)


def solution(mesh):
    placed = (
        P(None, "pulse", "range"),
        P(None, None, None, "pulse"),
        P(None, None, None, "pulse"),
        P(None, "pulse"),
    )
    return jax.shard_map(
        per_device, mesh=mesh, in_specs=placed, out_specs=P(None, "pulse", "range"), check_vma=False
    )
```

```python
import functools
import math

import jax
import jax.numpy as jnp
from jax import lax
from jax.experimental import pallas as pl
from jax.experimental.pallas import tpu as pltpu
from jax.sharding import PartitionSpec as P


BINS = 1024
BLOCK = 64
POWER = 3
MIB = 1024 * 1024
SMALL_LIMIT = 4
LANES = 128
EPSILON = 1e-06


F32 = jnp.float32
BF16 = jnp.bfloat16


SINE = (3.1415926401307077, -5.16771008350789, 2.550077523214589, -0.5982912856206265, 0.07765766030630428)
COSINE = (0.9999999532476085, -4.934792830619644, 4.058411352862619, -1.3318765680811142, 0.2196896110983216)


def cis_turns(turns):
    z = turns - jnp.floor(turns + 0.5)
    w = z * z
    s, c = SINE[-1], COSINE[-1]
    for more in SINE[-2::-1]:
        s = s * w + more
    for more in COSINE[-2::-1]:
        c = c * w + more
    s = s * z
    twice = s + s
    return 1.0 - twice * s, twice * c


def swap(block, axis, distance):
    count = lax.axis_size(axis)
    return lax.ppermute(block, axis, [(i, i ^ distance) for i in range(count)])


VMEM = pl.BlockSpec(memory_space=pltpu.VMEM)
SMEM = pl.BlockSpec(memory_space=pltpu.SMEM)
HBM = pl.BlockSpec(memory_space=pltpu.HBM)


def pack_kernel(taps, weights, squint, mine, near, far):
    def put(out, row, level, source):
        out[row : row + 4] = taps[level, source].astype(F32)
        out[row + 4 : row + 8] = weights[level, source].astype(F32)

    put(mine, 0, 0, 0)
    put(mine, 8, 0, 1)
    put(mine, 16, 1, 0)
    put(mine, 24, 2, 0)
    mine[32:35] = squint[...]
    mine[35:40] = jnp.zeros((5, mine.shape[1]), F32)
    put(near, 0, 1, 1)
    put(near, 8, 2, 0)
    near[16:19] = squint[...]
    near[19:24] = jnp.zeros((5, near.shape[1]), F32)
    put(far, 0, 2, 1)
    far[8:11] = squint[...]
    far[11:16] = jnp.zeros((5, far.shape[1]), F32)


def pack(taps, weights, squint):
    beams = squint.shape[1]
    return pl.pallas_call(
        pack_kernel,
        in_specs=[VMEM] * 3,
        out_specs=[VMEM] * 3,
        out_shape=[jax.ShapeDtypeStruct((rows, beams), F32) for rows in (40, 24, 16)],
        compiler_params=pltpu.CompilerParams(vmem_limit_bytes=SMALL_LIMIT * MIB),
        name="pack",
    )(taps, weights, squint)


def fill_matrices(columns, outs):
    beams = columns.shape[0]

    def part(i, _):
        at = pl.ds(pl.multiple_of(i * 16, 16), 16)
        lane = lax.broadcasted_iota(jnp.int32, (16, LANES), 1)
        lanes = [(lane + j * LANES).astype(jnp.int16) for j in range(beams // LANES)]
        whole = columns[at, :].astype(jnp.int32).astype(jnp.int16)
        real = columns[at, :].astype(BF16)

        def spread(value, column):
            return jnp.broadcast_to(value[:, column : column + 1], (16, LANES))

        for unit, out in enumerate(outs):
            taps = [spread(whole, 8 * unit + c) for c in range(4)]
            weights = [spread(real, 8 * unit + 4 + c) for c in range(4)]
            for j, here in enumerate(lanes):
                total = jnp.zeros((16, LANES), BF16)
                for tap, weight in zip(taps, weights):
                    total = jnp.where(here == tap, weight, total)
                out[at, j * LANES : (j + 1) * LANES] = total
        return 0

    lax.fori_loop(0, beams // 16, part, 0, unroll=2)


def first_kernel(pulses, scalars, mine, matrices, table, columns, rows):
    beams = matrices.shape[1]
    angles = beams * pulses
    classes = pulses // 2
    each = BINS // pulses
    rows[0:40] = mine[...]
    columns[...] = rows[...].T
    fill_matrices(columns, [matrices.at[u] for u in range(2)])
    count = BINS // classes
    inner = each // classes
    bits = pulses.bit_length() - 1

    def part(i, _):
        at = pl.ds(pl.multiple_of(i * 16, 16), 16)
        row = lax.broadcasted_iota(jnp.int32, (16, LANES), 0) + i * 16
        group = (row & (count - 1)) >> (inner.bit_length() - 1)
        mirrored = jnp.zeros_like(group)
        for bit in range(bits):
            mirrored = mirrored | ((group >> bit & 1) << (bits - 1 - bit))
        bins = (
            (mirrored ^ scalars[0]) * each
            + (row & (inner - 1)) * classes
            + (row >> (count.bit_length() - 1))
        )
        lane = lax.broadcasted_iota(jnp.int32, (16, LANES), 1)
        whole = angles - 1
        cosine, sine = cis_turns(
            (bins * (scalars[2] + lane & whole) & whole).astype(F32) * (1.0 / angles)
        )
        ahead_c, ahead_s = cis_turns((bins * LANES & whole).astype(F32) * (1.0 / angles))
        low = i * 16 + (i * 16 >> (count.bit_length() - 1)) * count
        cos_at = pl.ds(pl.multiple_of(low, 16), 16)
        sin_at = pl.ds(pl.multiple_of(low + count, 16), 16)
        for j in range(beams // LANES):
            lanes = slice(j * LANES, (j + 1) * LANES)
            table[cos_at, lanes] = cosine.astype(BF16)
            table[sin_at, lanes] = sine.astype(BF16)
            cosine, sine = (
                cosine * ahead_c - sine * ahead_s,
                sine * ahead_c + cosine * ahead_s,
            )
        return 0

    lax.fori_loop(0, BINS // 16, part, 0, unroll=2)


def first_tables(scalars, mine, pulses):
    beams = mine.shape[1]
    return pl.pallas_call(
        functools.partial(first_kernel, pulses),
        in_specs=[SMEM, VMEM],
        out_specs=[VMEM] * 2,
        out_shape=[
            jax.ShapeDtypeStruct((2, beams, beams), BF16),
            jax.ShapeDtypeStruct((2 * BINS, beams), BF16),
        ],
        scratch_shapes=[pltpu.VMEM((beams, LANES), F32), pltpu.VMEM((LANES, beams), F32)],
        compiler_params=pltpu.CompilerParams(vmem_limit_bytes=SMALL_LIMIT * MIB),
        cost_estimate=pl.CostEstimate(
            flops=4000 * beams * beams, bytes_accessed=8 * beams * beams, transcendentals=0
        ),
        name="first",
    )(scalars, mine)


def fetch(pulse_data, other, here, there, sems, start):
    return [
        pltpu.make_async_copy(
            source.at[t, :, pl.ds(start + j * LANES, LANES)],
            to.at[j, :, pl.ds(t * LANES, LANES)],
            sems.at[i, j, t],
        )
        for i, (source, to) in enumerate(((pulse_data, here), (other, there)))
        for j in range(here.shape[0])
        for t in range(2)
    ]


def second_kernel(
    ranges,
    scalars, mine, near, middle, far, pulse_data, other,
    split, join, phase, step, here, there,
    columns, rows, packs, sems,
):
    copies = fetch(pulse_data, other, here, there, sems, 0)
    for copy in copies:
        copy.start()
    beams = split.shape[1]
    place = scalars[1]
    packs[0, 0:8] = mine[24:32]
    packs[0, 8:16] = jnp.broadcast_to(mine[34:35], (8, beams))
    packs[1, 0:8] = near[8:16]
    packs[1, 8:16] = jnp.broadcast_to(near[18:19], (8, beams))
    packs[2, 0:8] = middle[0:8]
    packs[2, 8:16] = jnp.broadcast_to(middle[10:11], (8, beams))
    packs[3, 0:8] = far[0:8]
    packs[3, 8:16] = jnp.broadcast_to(far[10:11], (8, beams))
    packs[4, 0:8] = mine[16:24]
    packs[4, 8:16] = jnp.broadcast_to(mine[33:34], (8, beams))
    packs[5, 0:8] = near[0:8]
    packs[5, 8:16] = jnp.broadcast_to(near[17:18], (8, beams))
    order = [4 + (x ^ place & 1) for x in range(2)] + [k ^ place for k in range(4)]
    rows[48:56] = jnp.broadcast_to(mine[32:33], (8, beams))
    for unit, source in enumerate(order):
        rows[8 * unit : 8 * unit + 8] = packs[source, 0:8]
        rows[56 + 8 * unit : 64 + 8 * unit] = packs[source, 8:16]
    columns[...] = rows[...].T
    fill_matrices(
        columns, [split.at[u] for u in range(2)] + [join.at[u] for u in range(4)]
    )

    def part(i, _):
        at = pl.ds(pl.multiple_of(i * 16, 16), 16)
        p = columns[at, :]
        lane = lax.broadcasted_iota(jnp.int32, (16, LANES), 1)
        index = (lane + scalars[3]).astype(F32) * (1.0 / ranges)
        for unit in range(7):
            squint = p[:, 48 + 8 * unit : 49 + 8 * unit]
            cosine, sine = cis_turns(squint * index)
            phase[unit, 0, at, :] = cosine
            phase[unit, 1, at, :] = sine
        cosine, sine = cis_turns(p * (LANES / ranges))
        step[0, at, :] = cosine
        step[1, at, :] = sine
        return 0

    lax.fori_loop(0, beams // 16, part, 0, unroll=2)
    for copy in copies:
        copy.wait()


def second_tables(scalars, mine, near, middle, far, pulse_data, other, ranges, chunks):
    beams = mine.shape[1]
    return pl.pallas_call(
        functools.partial(second_kernel, ranges),
        in_specs=[SMEM] + [VMEM] * 4 + [HBM] * 2,
        out_specs=[VMEM] * 6,
        out_shape=[
            jax.ShapeDtypeStruct((2, beams, beams), BF16),
            jax.ShapeDtypeStruct((4, beams, beams), BF16),
            jax.ShapeDtypeStruct((7, 2, beams, LANES), F32),
            jax.ShapeDtypeStruct((2, beams, LANES), F32),
            jax.ShapeDtypeStruct((chunks, beams, 2 * LANES), BF16),
            jax.ShapeDtypeStruct((chunks, beams, 2 * LANES), BF16),
        ],
        scratch_shapes=[
            pltpu.VMEM((beams, LANES), F32),
            pltpu.VMEM((LANES, beams), F32),
            pltpu.VMEM((6, 16, beams), F32),
            pltpu.SemaphoreType.DMA((2, chunks, 2)),
        ],
        compiler_params=pltpu.CompilerParams(vmem_limit_bytes=SMALL_LIMIT * MIB),
        cost_estimate=pl.CostEstimate(
            flops=8000 * beams * beams, bytes_accessed=12 * beams * beams, transcendentals=0
        ),
        name="second",
    )(scalars, mine, near, middle, far, pulse_data, other)


def turned(base, value, turn, count):
    c = math.cos(2.0 * math.pi * turn / count)
    s = math.sin(2.0 * math.pi * turn / count)
    real, imag = base
    re, im = value
    for amount, add_re, add_im in ((c, re, im), (s, im, -re)):
        if abs(amount) < 1e-9:
            continue
        if abs(abs(amount) - 1.0) > 1e-9:
            real, imag = real + amount * add_re, imag + amount * add_im
        elif amount > 0.0:
            real, imag = real + add_re, imag + add_im
        else:
            real, imag = real - add_re, imag - add_im
    return real, imag


def main_limit(classes):
    return (7 if classes <= 4 else 40) * MIB


def main_kernel(
    start, classes, more,
    near, far, merge, split, join, azimuth, step, phase_in,
    *refs,
):
    if more:
        pulse_data, other, keep, send, phase, here, there, merged, pair, spread, sems = refs
        copies = fetch(pulse_data, other, here, there, sems, start)
    else:
        keep, send, phase, merged, pair, spread = refs
        copies = []
    for copy in copies:
        copy.start()
    beams = merged.shape[0]
    tile = 512
    tiles = beams // tile
    small = 256

    def rotate(unit, at, total):
        cosine = phase[unit, 0, at, :]
        sine = phase[unit, 1, at, :]
        ahead_c = step[0, at, 48 + 8 * unit : 49 + 8 * unit]
        ahead_s = step[1, at, 48 + 8 * unit : 49 + 8 * unit]
        phase[unit, 0, at, :] = cosine * ahead_c - sine * ahead_s
        phase[unit, 1, at, :] = cosine * ahead_s + sine * ahead_c
        real = total[:, :LANES]
        imag = total[:, LANES:]
        return cosine * real - sine * imag, sine * real + cosine * imag

    def product(lhs, rhs):
        return jnp.dot(lhs, rhs, preferred_element_type=F32)

    def chunk(j, _):
        lanes = pl.ds(pl.multiple_of(j * LANES, LANES), LANES)
        for i in range(tiles):
            at = pl.ds(i * tile, tile)
            real, imag = rotate(
                0, at, product(merge[0, at, :], near[j]) + product(merge[1, at, :], far[j])
            )
            merged[at, :LANES] = real.astype(BF16)
            merged[at, LANES:] = imag.astype(BF16)
        for x in range(2):
            for i in range(tiles):
                at = pl.ds(i * tile, tile)
                real, imag = rotate(1 + x, at, product(split[x, at, :], merged[...]))
                pair[x, at, :LANES] = real.astype(BF16)
                pair[x, at, LANES:] = imag.astype(BF16)
        for i in range(beams // small):
            at = pl.ds(i * small, small)
            terms = [
                rotate(3 + k, at, product(join[k, at, :], pair[k % 2])) for k in range(4)
            ]
            pairs = {}
            for q in range(classes):
                turn = 2 * q % classes
                if turn not in pairs:
                    pairs[turn] = [turned(terms[x], terms[x + 2], turn, classes) for x in range(2)]
                real, imag = turned(*pairs[turn], q, classes)
                spread[q, at, :LANES] = real.astype(BF16)
                spread[q, at, LANES:] = imag.astype(BF16)
        rows = BINS // classes
        half = rows // 2
        for q in range(classes):
            both = product(azimuth[pl.ds(2 * q * rows, 2 * rows), :], spread[q])
            by_cos, by_sin = both[:rows], both[rows:]
            sides = (
                by_cos[:, :LANES] + by_sin[:, LANES:],
                by_cos[:, LANES:] - by_sin[:, :LANES],
            )
            for t, side in enumerate(sides):
                keep[t, q, :, lanes] = side[:half]
                send[t, q, :, lanes] = side[half:].astype(BF16)
        return 0

    lax.fori_loop(0, near.shape[0], chunk, 0)
    for copy in copies:
        copy.wait()


def partial_spectrum(near, far, tables, phase, pulse_data, other, start, chunks, classes):
    beams = near.shape[1]
    width = near.shape[0] * LANES
    half = BINS // classes // 2
    ahead = [jax.ShapeDtypeStruct((chunks, beams, 2 * LANES), BF16)] * 2 if chunks else []
    return pl.pallas_call(
        functools.partial(main_kernel, start, classes, chunks > 0),
        in_specs=[VMEM] * 8 + [HBM] * len(ahead),
        out_specs=[VMEM] * (3 + len(ahead)),
        out_shape=[
            jax.ShapeDtypeStruct((2, classes, half, width), F32),
            jax.ShapeDtypeStruct((2, classes, half, width), BF16),
            jax.ShapeDtypeStruct(phase.shape, F32),
        ]
        + ahead,
        scratch_shapes=[
            pltpu.VMEM((beams, 2 * LANES), BF16),
            pltpu.VMEM((2, beams, 2 * LANES), BF16),
            pltpu.VMEM((classes, beams, 2 * LANES), BF16),
        ]
        + ([pltpu.SemaphoreType.DMA((2, chunks, 2))] if ahead else []),
        input_output_aliases={7: 2},
        compiler_params=pltpu.CompilerParams(vmem_limit_bytes=main_limit(classes)),
        cost_estimate=pl.CostEstimate(
            flops=2 * 20 * beams * beams * width,
            bytes_accessed=beams * beams,
            transcendentals=0,
        ),
        name="main",
    )(near, far, *tables, phase, *([pulse_data, other] if ahead else []))


def covariance_kernel(scale, *refs):
    parts = (len(refs) - 2) // 2
    kept, received = refs[:parts], refs[parts : 2 * parts]
    spectrum, covariance = refs[2 * parts :]
    classes, rows = kept[0].shape[1:3]
    inner = BLOCK // classes
    at = 0
    for h in range(parts):
        width = kept[h].shape[3]
        spectrum[:, :, :, at : at + width] = (
            kept[h][...] + received[h][...].astype(F32)
        ) * scale
        at += width

    def gram(a, b):
        return lax.dot_general(
            a, b, (((1,), (1,)), ((), ())),
            precision=lax.Precision.HIGHEST, preferred_element_type=F32,
        )

    def block(b, _):
        at = pl.ds(pl.multiple_of(b * inner, inner), inner)
        real, imag = [
            jnp.concatenate([spectrum[t, q, at, :] for q in range(classes)], axis=0)
            for t in range(2)
        ]
        covariance[b] = gram(real, jnp.concatenate([real, -imag], axis=0)) + gram(
            imag, jnp.concatenate([imag, real], axis=0)
        )
        return 0

    lax.fori_loop(0, rows // inner, block, 0)


def spectrum_and_covariance(kept, received, scale):
    _, classes, rows, _ = kept[0].shape
    width = sum(part.shape[3] for part in kept)
    inner = BLOCK // classes
    return pl.pallas_call(
        functools.partial(covariance_kernel, scale),
        in_specs=[VMEM] * (2 * len(kept)),
        out_specs=[VMEM, VMEM],
        out_shape=[
            jax.ShapeDtypeStruct((2, classes, rows, width), F32),
            jax.ShapeDtypeStruct((rows // inner, BLOCK, 2 * BLOCK), F32),
        ],
        compiler_params=pltpu.CompilerParams(vmem_limit_bytes=SMALL_LIMIT * MIB),
        name="covariance",
    )(*kept, *received)


def focus_kernel(*refs):
    covs, (spectrum, out, stage) = refs[:-3], refs[-3:]
    classes, rows = spectrum.shape[1:3]
    inner = BLOCK // classes
    factor = math.sqrt(BLOCK)
    lane = lax.broadcasted_iota(jnp.int32, (1, 2 * BLOCK), 1)
    first = lane < BLOCK

    def turned(row):
        return pltpu.roll(jnp.broadcast_to(row, (8, 2 * BLOCK)), BLOCK, 1)[0:1]

    for b in range(rows // inner):
        cov = covs[0][b]
        for other in covs[1:]:
            cov = cov + other[b]
        vec_re = jnp.where(first, 1.0, 0.0)
        vec_im = jnp.zeros((1, 2 * BLOCK), F32)
        for step in range(POWER):
            if step % 2 == 0:
                new_re = jnp.sum(
                    cov * jnp.where(first, vec_re, -turned(vec_im)), axis=1, keepdims=True
                )
                new_im = jnp.sum(
                    cov * jnp.where(first, vec_im, turned(vec_re)), axis=1, keepdims=True
                )
                power = jnp.sum(new_re * new_re + new_im * new_im, axis=0, keepdims=True)
            else:
                by_re = jnp.sum(cov * vec_re, axis=0, keepdims=True)
                by_im = jnp.sum(cov * vec_im, axis=0, keepdims=True)
                new_re = jnp.where(first, by_re + turned(by_im), 0.0)
                new_im = jnp.where(first, by_im - turned(by_re), 0.0)
                power = jnp.sum(new_re * new_re + new_im * new_im, axis=1, keepdims=True)
            length = jnp.sqrt(power + EPSILON)
            vec_re = new_re / length
            vec_im = new_im / length
        for q in range(classes):
            re = spectrum[0, q, b * inner : (b + 1) * inner, :]
            im = spectrum[1, q, b * inner : (b + 1) * inner, :]
            by_re = vec_re[q * inner : (q + 1) * inner] * factor
            by_im = vec_im[q * inner : (q + 1) * inner] * factor
            at = pl.ds(q, inner, stride=classes)
            for t, side in enumerate((re * by_re + im * by_im, im * by_re - re * by_im)):
                for j in range(stage.shape[1]):
                    stage[t, j, at, :] = side[:, j * LANES : (j + 1) * LANES]
        for t in range(2):
            for j in range(stage.shape[1]):
                out[t, b * BLOCK : (b + 1) * BLOCK, j * LANES : (j + 1) * LANES] = stage[t, j]


def focus(covs, spectrum):
    _, classes, rows, ranges = spectrum.shape
    return pl.pallas_call(
        focus_kernel,
        in_specs=[VMEM] * (len(covs) + 1),
        out_specs=VMEM,
        out_shape=jax.ShapeDtypeStruct((2, classes * rows, ranges), F32),
        scratch_shapes=[pltpu.VMEM((2, ranges // LANES, BLOCK, LANES), F32)],
        compiler_params=pltpu.CompilerParams(vmem_limit_bytes=SMALL_LIMIT * MIB),
        name="focus",
    )(*covs, spectrum)


def per_device(pulse_data, merge_taps, merge_weights, squint):
    pulses = lax.axis_size("pulse")
    range_count = lax.axis_size("range")
    pulse_index = lax.axis_index("pulse")
    range_index = lax.axis_index("range")
    _, beams, range_cols = pulse_data.shape
    ranges = range_cols * range_count
    angles = beams * pulses
    classes = pulses // 2
    mine, near, far = pack(merge_taps, merge_weights, squint)
    near = swap(near, "pulse", 2)
    middle = swap(far, "pulse", 4)
    far = swap(far, "pulse", 6)
    other = swap(pulse_data, "pulse", 1)
    scalars = jnp.stack(
        [
            pulse_index,
            pulse_index >> 1 & 3,
            (pulse_index & ~6) * beams,
            range_index * range_cols,
        ]
    )
    merge, azimuth = first_tables(scalars, mine, pulses)
    total = range_cols // LANES
    sizes = [total // 4, total // 4, total // 4, total - total // 8 * 7, total // 8] if total >= 8 else [1] * total
    calls = len(sizes)
    split, join, phase, step, here, there = second_tables(
        scalars, mine, near, middle, far, pulse_data, other, ranges, sizes[0]
    )
    tables = (merge, split, join, azimuth, step)
    stages = pulses.bit_length() - 1
    halves = [None] * calls

    def advance(part):
        keep, arrived, stage = halves[part]
        total = keep + arrived.astype(F32)
        half = total.shape[2] // 2
        send = total[:, :, half:].astype(BF16)
        arrived = swap(send, "pulse", 1 << stage)
        halves[part] = (total[:, :, :half], arrived, stage + 1)
        return send

    for part in range(calls):
        done = [advance(p) for p in range(part - 1) if halves[p][2] < stages]
        if done:
            phase, done = lax.optimization_barrier((phase, done))
        keep, send, phase, *ahead = partial_spectrum(
            here, there, tables, phase, pulse_data, other,
            sum(sizes[: part + 1]) * LANES,
            sizes[part + 1] if part + 1 < calls else 0,
            classes,
        )
        if ahead:
            here, there = ahead
        halves[part] = (keep, swap(send, "pulse", 1), 1)
    for stage in range(1, stages):
        for part in range(calls):
            if halves[part][2] == stage:
                advance(part)
    kept = [half[0] for half in halves]
    received = [half[1] for half in halves]
    spectrum, cov = spectrum_and_covariance(kept, received, angles ** (-0.5))
    covs = [cov]
    distance = 1
    while distance < range_count:
        total = covs[0]
        for extra in covs[1:]:
            total = total + extra
        covs = [total]
        for turn in range(1, min(4, range_count // distance)):
            covs.append(swap(total, "range", turn * distance))
        distance *= 4
    return focus(covs, spectrum)


def solution(mesh):
    placed = (
        P(None, "pulse", "range"),
        P(None, None, None, "pulse"),
        P(None, None, None, "pulse"),
        P(None, "pulse"),
    )
    return jax.shard_map(
        per_device, mesh=mesh, in_specs=placed, out_specs=P(None, "pulse", "range"), check_vma=False
    )
```

```python
import functools
import math

import jax
import jax.numpy as jnp
from jax import lax
from jax.experimental import pallas as pl
from jax.experimental.pallas import tpu as pltpu
from jax.sharding import PartitionSpec as P


BINS = 1024
BLOCK = 64
POWER = 3
MIB = 1024 * 1024
SMALL_LIMIT = 4
LANES = 128
EPSILON = 1e-06


F32 = jnp.float32
BF16 = jnp.bfloat16


SINE = (3.1415926401307077, -5.16771008350789, 2.550077523214589, -0.5982912856206265, 0.07765766030630428)
COSINE = (0.9999999532476085, -4.934792830619644, 4.058411352862619, -1.3318765680811142, 0.2196896110983216)


def cis_turns(turns):
    z = turns - jnp.floor(turns + 0.5)
    w = z * z
    s, c = SINE[-1], COSINE[-1]
    for more in SINE[-2::-1]:
        s = s * w + more
    for more in COSINE[-2::-1]:
        c = c * w + more
    s = s * z
    twice = s + s
    return 1.0 - twice * s, twice * c


def swap(block, axis, distance):
    count = lax.axis_size(axis)
    return lax.ppermute(block, axis, [(i, i ^ distance) for i in range(count)])


VMEM = pl.BlockSpec(memory_space=pltpu.VMEM)
SMEM = pl.BlockSpec(memory_space=pltpu.SMEM)
HBM = pl.BlockSpec(memory_space=pltpu.HBM)


def pack_kernel(taps, weights, squint, mine, near, far):
    def put(out, row, level, source):
        out[row : row + 4] = taps[level, source].astype(F32)
        out[row + 4 : row + 8] = weights[level, source].astype(F32)

    put(mine, 0, 0, 0)
    put(mine, 8, 0, 1)
    put(mine, 16, 1, 0)
    put(mine, 24, 2, 0)
    mine[32:35] = squint[...]
    mine[35:40] = jnp.zeros((5, mine.shape[1]), F32)
    put(near, 0, 1, 1)
    put(near, 8, 2, 0)
    near[16:19] = squint[...]
    near[19:24] = jnp.zeros((5, near.shape[1]), F32)
    put(far, 0, 2, 1)
    far[8:11] = squint[...]
    far[11:16] = jnp.zeros((5, far.shape[1]), F32)


def pack(taps, weights, squint):
    beams = squint.shape[1]
    return pl.pallas_call(
        pack_kernel,
        in_specs=[VMEM] * 3,
        out_specs=[VMEM] * 3,
        out_shape=[jax.ShapeDtypeStruct((rows, beams), F32) for rows in (40, 24, 16)],
        compiler_params=pltpu.CompilerParams(vmem_limit_bytes=SMALL_LIMIT * MIB),
        name="pack",
    )(taps, weights, squint)


def fill_matrices(columns, outs):
    beams = columns.shape[0]

    def part(i, _):
        at = pl.ds(pl.multiple_of(i * 16, 16), 16)
        lane = lax.broadcasted_iota(jnp.int32, (16, LANES), 1)
        lanes = [(lane + j * LANES).astype(jnp.int16) for j in range(beams // LANES)]
        whole = columns[at, :].astype(jnp.int32).astype(jnp.int16)
        real = columns[at, :].astype(BF16)

        def spread(value, column):
            return jnp.broadcast_to(value[:, column : column + 1], (16, LANES))

        for unit, out in enumerate(outs):
            taps = [spread(whole, 8 * unit + c) for c in range(4)]
            weights = [spread(real, 8 * unit + 4 + c) for c in range(4)]
            for j, here in enumerate(lanes):
                total = jnp.zeros((16, LANES), BF16)
                for tap, weight in zip(taps, weights):
                    total = jnp.where(here == tap, weight, total)
                out[at, j * LANES : (j + 1) * LANES] = total
        return 0

    lax.fori_loop(0, beams // 16, part, 0, unroll=2)


def first_kernel(pulses, scalars, mine, matrices, table, columns, rows):
    beams = matrices.shape[1]
    angles = beams * pulses
    classes = pulses // 2
    each = BINS // pulses
    rows[0:40] = mine[...]
    columns[...] = rows[...].T
    fill_matrices(columns, [matrices.at[u] for u in range(2)])
    count = BINS // classes
    inner = each // classes
    bits = pulses.bit_length() - 1

    def part(i, _):
        at = pl.ds(pl.multiple_of(i * 16, 16), 16)
        row = lax.broadcasted_iota(jnp.int32, (16, LANES), 0) + i * 16
        group = (row & (count - 1)) >> (inner.bit_length() - 1)
        mirrored = jnp.zeros_like(group)
        for bit in range(bits):
            mirrored = mirrored | ((group >> bit & 1) << (bits - 1 - bit))
        bins = (
            (mirrored ^ scalars[0]) * each
            + (row & (inner - 1)) * classes
            + (row >> (count.bit_length() - 1))
        )
        lane = lax.broadcasted_iota(jnp.int32, (16, LANES), 1)
        whole = angles - 1
        cosine, sine = cis_turns(
            (bins * (scalars[2] + lane & whole) & whole).astype(F32) * (1.0 / angles)
        )
        ahead_c, ahead_s = cis_turns((bins * LANES & whole).astype(F32) * (1.0 / angles))
        low = i * 16 + (i * 16 >> (count.bit_length() - 1)) * count
        cos_at = pl.ds(pl.multiple_of(low, 16), 16)
        sin_at = pl.ds(pl.multiple_of(low + count, 16), 16)
        for j in range(beams // LANES):
            lanes = slice(j * LANES, (j + 1) * LANES)
            table[cos_at, lanes] = cosine.astype(BF16)
            table[sin_at, lanes] = sine.astype(BF16)
            cosine, sine = (
                cosine * ahead_c - sine * ahead_s,
                sine * ahead_c + cosine * ahead_s,
            )
        return 0

    lax.fori_loop(0, BINS // 16, part, 0, unroll=2)


def first_tables(scalars, mine, pulses):
    beams = mine.shape[1]
    return pl.pallas_call(
        functools.partial(first_kernel, pulses),
        in_specs=[SMEM, VMEM],
        out_specs=[VMEM] * 2,
        out_shape=[
            jax.ShapeDtypeStruct((2, beams, beams), BF16),
            jax.ShapeDtypeStruct((2 * BINS, beams), BF16),
        ],
        scratch_shapes=[pltpu.VMEM((beams, LANES), F32), pltpu.VMEM((LANES, beams), F32)],
        compiler_params=pltpu.CompilerParams(vmem_limit_bytes=SMALL_LIMIT * MIB),
        cost_estimate=pl.CostEstimate(
            flops=4000 * beams * beams, bytes_accessed=8 * beams * beams, transcendentals=0
        ),
        name="first",
    )(scalars, mine)


def fetch(pulse_data, other, here, there, sems, start):
    return [
        pltpu.make_async_copy(
            source.at[t, :, pl.ds(start + j * LANES, LANES)],
            to.at[j, :, pl.ds(t * LANES, LANES)],
            sems.at[i, j, t],
        )
        for i, (source, to) in enumerate(((pulse_data, here), (other, there)))
        for j in range(here.shape[0])
        for t in range(2)
    ]


def second_kernel(
    ranges,
    scalars, mine, near, middle, far, pulse_data, other,
    split, join, phase, step, here, there,
    columns, rows, packs, sems,
):
    copies = fetch(pulse_data, other, here, there, sems, 0)
    for copy in copies:
        copy.start()
    beams = split.shape[1]
    place = scalars[1]
    packs[0, 0:8] = mine[24:32]
    packs[0, 8:16] = jnp.broadcast_to(mine[34:35], (8, beams))
    packs[1, 0:8] = near[8:16]
    packs[1, 8:16] = jnp.broadcast_to(near[18:19], (8, beams))
    packs[2, 0:8] = middle[0:8]
    packs[2, 8:16] = jnp.broadcast_to(middle[10:11], (8, beams))
    packs[3, 0:8] = far[0:8]
    packs[3, 8:16] = jnp.broadcast_to(far[10:11], (8, beams))
    packs[4, 0:8] = mine[16:24]
    packs[4, 8:16] = jnp.broadcast_to(mine[33:34], (8, beams))
    packs[5, 0:8] = near[0:8]
    packs[5, 8:16] = jnp.broadcast_to(near[17:18], (8, beams))
    order = [4 + (x ^ place & 1) for x in range(2)] + [k ^ place for k in range(4)]
    rows[48:56] = jnp.broadcast_to(mine[32:33], (8, beams))
    for unit, source in enumerate(order):
        rows[8 * unit : 8 * unit + 8] = packs[source, 0:8]
        rows[56 + 8 * unit : 64 + 8 * unit] = packs[source, 8:16]
    columns[...] = rows[...].T
    fill_matrices(
        columns, [split.at[u] for u in range(2)] + [join.at[u] for u in range(4)]
    )

    def part(i, _):
        at = pl.ds(pl.multiple_of(i * 16, 16), 16)
        p = columns[at, :]
        lane = lax.broadcasted_iota(jnp.int32, (16, LANES), 1)
        index = (lane + scalars[3]).astype(F32) * (1.0 / ranges)
        for unit in range(7):
            squint = p[:, 48 + 8 * unit : 49 + 8 * unit]
            cosine, sine = cis_turns(squint * index)
            phase[unit, 0, at, :] = cosine
            phase[unit, 1, at, :] = sine
        cosine, sine = cis_turns(p * (LANES / ranges))
        step[0, at, :] = cosine
        step[1, at, :] = sine
        return 0

    lax.fori_loop(0, beams // 16, part, 0, unroll=2)
    for copy in copies:
        copy.wait()


def second_tables(scalars, mine, near, middle, far, pulse_data, other, ranges, chunks):
    beams = mine.shape[1]
    return pl.pallas_call(
        functools.partial(second_kernel, ranges),
        in_specs=[SMEM] + [VMEM] * 4 + [HBM] * 2,
        out_specs=[VMEM] * 6,
        out_shape=[
            jax.ShapeDtypeStruct((2, beams, beams), BF16),
            jax.ShapeDtypeStruct((4, beams, beams), BF16),
            jax.ShapeDtypeStruct((7, 2, beams, LANES), F32),
            jax.ShapeDtypeStruct((2, beams, LANES), F32),
            jax.ShapeDtypeStruct((chunks, beams, 2 * LANES), BF16),
            jax.ShapeDtypeStruct((chunks, beams, 2 * LANES), BF16),
        ],
        scratch_shapes=[
            pltpu.VMEM((beams, LANES), F32),
            pltpu.VMEM((LANES, beams), F32),
            pltpu.VMEM((6, 16, beams), F32),
            pltpu.SemaphoreType.DMA((2, chunks, 2)),
        ],
        compiler_params=pltpu.CompilerParams(vmem_limit_bytes=SMALL_LIMIT * MIB),
        cost_estimate=pl.CostEstimate(
            flops=8000 * beams * beams, bytes_accessed=12 * beams * beams, transcendentals=0
        ),
        name="second",
    )(scalars, mine, near, middle, far, pulse_data, other)


def turned(base, value, turn, count):
    c = math.cos(2.0 * math.pi * turn / count)
    s = math.sin(2.0 * math.pi * turn / count)
    real, imag = base
    re, im = value
    for amount, add_re, add_im in ((c, re, im), (s, im, -re)):
        if abs(amount) < 1e-9:
            continue
        if abs(abs(amount) - 1.0) > 1e-9:
            real, imag = real + amount * add_re, imag + amount * add_im
        elif amount > 0.0:
            real, imag = real + add_re, imag + add_im
        else:
            real, imag = real - add_re, imag - add_im
    return real, imag


def main_limit(classes):
    return (7 if classes <= 4 else 40) * MIB


def main_kernel(
    start, classes, more,
    near, far, merge, split, join, azimuth, step, phase_in,
    *refs,
):
    if more:
        pulse_data, other, keep, send, phase, here, there, merged, pair, spread, sems = refs
        copies = fetch(pulse_data, other, here, there, sems, start)
    else:
        keep, send, phase, merged, pair, spread = refs
        copies = []
    for copy in copies:
        copy.start()
    beams = merged.shape[0]
    tile = 512
    tiles = beams // tile
    small = 256

    def rotate(unit, at, total):
        cosine = phase[unit, 0, at, :]
        sine = phase[unit, 1, at, :]
        if more or near.shape[0] > 1:
            ahead_c = step[0, at, 48 + 8 * unit : 49 + 8 * unit]
            ahead_s = step[1, at, 48 + 8 * unit : 49 + 8 * unit]
            phase[unit, 0, at, :] = cosine * ahead_c - sine * ahead_s
            phase[unit, 1, at, :] = cosine * ahead_s + sine * ahead_c
        real = total[:, :LANES]
        imag = total[:, LANES:]
        return cosine * real - sine * imag, sine * real + cosine * imag

    def product(lhs, rhs):
        return jnp.dot(lhs, rhs, preferred_element_type=F32)

    def chunk(j, _):
        lanes = pl.ds(pl.multiple_of(j * LANES, LANES), LANES)
        for i in range(tiles):
            at = pl.ds(i * tile, tile)
            real, imag = rotate(
                0, at, product(merge[0, at, :], near[j]) + product(merge[1, at, :], far[j])
            )
            merged[at, :LANES] = real.astype(BF16)
            merged[at, LANES:] = imag.astype(BF16)
        for x in range(2):
            for i in range(tiles):
                at = pl.ds(i * tile, tile)
                real, imag = rotate(1 + x, at, product(split[x, at, :], merged[...]))
                pair[x, at, :LANES] = real.astype(BF16)
                pair[x, at, LANES:] = imag.astype(BF16)
        for i in range(beams // small):
            at = pl.ds(i * small, small)
            terms = [
                rotate(3 + k, at, product(join[k, at, :], pair[k % 2])) for k in range(4)
            ]
            pairs = {}
            for q in range(classes):
                turn = 2 * q % classes
                if turn not in pairs:
                    pairs[turn] = [turned(terms[x], terms[x + 2], turn, classes) for x in range(2)]
                real, imag = turned(*pairs[turn], q, classes)
                spread[q, at, :LANES] = real.astype(BF16)
                spread[q, at, LANES:] = imag.astype(BF16)
        rows = BINS // classes
        half = rows // 2
        for q in range(classes):
            both = product(azimuth[pl.ds(2 * q * rows, 2 * rows), :], spread[q])
            by_cos, by_sin = both[:rows], both[rows:]
            sides = (
                by_cos[:, :LANES] + by_sin[:, LANES:],
                by_cos[:, LANES:] - by_sin[:, :LANES],
            )
            for t, side in enumerate(sides):
                keep[t, q, :, lanes] = side[:half]
                send[t, q, :, lanes] = side[half:].astype(BF16)
        return 0

    lax.fori_loop(0, near.shape[0], chunk, 0)
    for copy in copies:
        copy.wait()


def partial_spectrum(near, far, tables, phase, pulse_data, other, start, chunks, classes):
    beams = near.shape[1]
    width = near.shape[0] * LANES
    half = BINS // classes // 2
    ahead = [jax.ShapeDtypeStruct((chunks, beams, 2 * LANES), BF16)] * 2 if chunks else []
    return pl.pallas_call(
        functools.partial(main_kernel, start, classes, chunks > 0),
        in_specs=[VMEM] * 8 + [HBM] * len(ahead),
        out_specs=[VMEM] * (3 + len(ahead)),
        out_shape=[
            jax.ShapeDtypeStruct((2, classes, half, width), F32),
            jax.ShapeDtypeStruct((2, classes, half, width), BF16),
            jax.ShapeDtypeStruct(phase.shape, F32),
        ]
        + ahead,
        scratch_shapes=[
            pltpu.VMEM((beams, 2 * LANES), BF16),
            pltpu.VMEM((2, beams, 2 * LANES), BF16),
            pltpu.VMEM((classes, beams, 2 * LANES), BF16),
        ]
        + ([pltpu.SemaphoreType.DMA((2, chunks, 2))] if ahead else []),
        input_output_aliases={7: 2},
        compiler_params=pltpu.CompilerParams(vmem_limit_bytes=main_limit(classes)),
        cost_estimate=pl.CostEstimate(
            flops=2 * 20 * beams * beams * width,
            bytes_accessed=beams * beams,
            transcendentals=0,
        ),
        name="main",
    )(near, far, *tables, phase, *([pulse_data, other] if ahead else []))


def covariance_kernel(scale, *refs):
    parts = (len(refs) - 2) // 2
    kept, received = refs[:parts], refs[parts : 2 * parts]
    spectrum, covariance = refs[2 * parts :]
    classes, rows = kept[0].shape[1:3]
    inner = BLOCK // classes
    at = 0
    for h in range(parts):
        width = kept[h].shape[3]
        spectrum[:, :, :, at : at + width] = (
            kept[h][...] + received[h][...].astype(F32)
        ) * scale
        at += width

    def gram(a, b):
        return lax.dot_general(
            a, b, (((1,), (1,)), ((), ())),
            precision=lax.Precision.HIGHEST, preferred_element_type=F32,
        )

    def block(b, _):
        at = pl.ds(pl.multiple_of(b * inner, inner), inner)
        real, imag = [
            jnp.concatenate([spectrum[t, q, at, :] for q in range(classes)], axis=0)
            for t in range(2)
        ]
        covariance[b] = gram(real, jnp.concatenate([real, -imag], axis=0)) + gram(
            imag, jnp.concatenate([imag, real], axis=0)
        )
        return 0

    lax.fori_loop(0, rows // inner, block, 0)


def spectrum_and_covariance(kept, received, scale):
    _, classes, rows, _ = kept[0].shape
    width = sum(part.shape[3] for part in kept)
    inner = BLOCK // classes
    return pl.pallas_call(
        functools.partial(covariance_kernel, scale),
        in_specs=[VMEM] * (2 * len(kept)),
        out_specs=[VMEM, VMEM],
        out_shape=[
            jax.ShapeDtypeStruct((2, classes, rows, width), F32),
            jax.ShapeDtypeStruct((rows // inner, BLOCK, 2 * BLOCK), F32),
        ],
        compiler_params=pltpu.CompilerParams(vmem_limit_bytes=SMALL_LIMIT * MIB),
        name="covariance",
    )(*kept, *received)


def focus_kernel(*refs):
    covs, (spectrum, out, stage) = refs[:-3], refs[-3:]
    classes, rows = spectrum.shape[1:3]
    inner = BLOCK // classes
    factor = math.sqrt(BLOCK)
    lane = lax.broadcasted_iota(jnp.int32, (1, 2 * BLOCK), 1)
    first = lane < BLOCK

    def turned(row):
        return pltpu.roll(jnp.broadcast_to(row, (8, 2 * BLOCK)), BLOCK, 1)[0:1]

    for b in range(rows // inner):
        cov = covs[0][b]
        for other in covs[1:]:
            cov = cov + other[b]
        vec_re = jnp.where(first, 1.0, 0.0)
        vec_im = jnp.zeros((1, 2 * BLOCK), F32)
        for step in range(POWER):
            if step % 2 == 0:
                new_re = jnp.sum(
                    cov * jnp.where(first, vec_re, -turned(vec_im)), axis=1, keepdims=True
                )
                new_im = jnp.sum(
                    cov * jnp.where(first, vec_im, turned(vec_re)), axis=1, keepdims=True
                )
                power = jnp.sum(new_re * new_re + new_im * new_im, axis=0, keepdims=True)
            else:
                by_re = jnp.sum(cov * vec_re, axis=0, keepdims=True)
                by_im = jnp.sum(cov * vec_im, axis=0, keepdims=True)
                new_re = jnp.where(first, by_re + turned(by_im), 0.0)
                new_im = jnp.where(first, by_im - turned(by_re), 0.0)
                power = jnp.sum(new_re * new_re + new_im * new_im, axis=1, keepdims=True)
            length = jnp.sqrt(power + EPSILON)
            vec_re = new_re / length
            vec_im = new_im / length
        for q in range(classes):
            re = spectrum[0, q, b * inner : (b + 1) * inner, :]
            im = spectrum[1, q, b * inner : (b + 1) * inner, :]
            by_re = vec_re[q * inner : (q + 1) * inner] * factor
            by_im = vec_im[q * inner : (q + 1) * inner] * factor
            at = pl.ds(q, inner, stride=classes)
            for t, side in enumerate((re * by_re + im * by_im, im * by_re - re * by_im)):
                for j in range(stage.shape[1]):
                    stage[t, j, at, :] = side[:, j * LANES : (j + 1) * LANES]
        for t in range(2):
            for j in range(stage.shape[1]):
                out[t, b * BLOCK : (b + 1) * BLOCK, j * LANES : (j + 1) * LANES] = stage[t, j]


def focus(covs, spectrum):
    _, classes, rows, ranges = spectrum.shape
    return pl.pallas_call(
        focus_kernel,
        in_specs=[VMEM] * (len(covs) + 1),
        out_specs=VMEM,
        out_shape=jax.ShapeDtypeStruct((2, classes * rows, ranges), F32),
        scratch_shapes=[pltpu.VMEM((2, ranges // LANES, BLOCK, LANES), F32)],
        compiler_params=pltpu.CompilerParams(vmem_limit_bytes=SMALL_LIMIT * MIB),
        name="focus",
    )(*covs, spectrum)


def per_device(pulse_data, merge_taps, merge_weights, squint):
    pulses = lax.axis_size("pulse")
    range_count = lax.axis_size("range")
    pulse_index = lax.axis_index("pulse")
    range_index = lax.axis_index("range")
    _, beams, range_cols = pulse_data.shape
    ranges = range_cols * range_count
    angles = beams * pulses
    classes = pulses // 2
    mine, near, far = pack(merge_taps, merge_weights, squint)
    near = swap(near, "pulse", 2)
    middle = swap(far, "pulse", 4)
    far = swap(far, "pulse", 6)
    other = swap(pulse_data, "pulse", 1)
    scalars = jnp.stack(
        [
            pulse_index,
            pulse_index >> 1 & 3,
            (pulse_index & ~6) * beams,
            range_index * range_cols,
        ]
    )
    merge, azimuth = first_tables(scalars, mine, pulses)
    total = range_cols // LANES
    sizes = [total // 4, total // 4, total // 4, total - total // 8 * 7, total // 8] if total >= 8 else [1] * total
    calls = len(sizes)
    split, join, phase, step, here, there = second_tables(
        scalars, mine, near, middle, far, pulse_data, other, ranges, sizes[0]
    )
    tables = (merge, split, join, azimuth, step)
    stages = pulses.bit_length() - 1
    halves = [None] * calls

    def advance(part):
        keep, arrived, stage = halves[part]
        total = keep + arrived.astype(F32)
        half = total.shape[2] // 2
        send = total[:, :, half:].astype(BF16)
        arrived = swap(send, "pulse", 1 << stage)
        halves[part] = (total[:, :, :half], arrived, stage + 1)
        return send

    def advance_together(parts):
        stage = stages - 1
        total = jnp.concatenate([halves[p][0] + halves[p][1].astype(F32) for p in parts], axis=3)
        half = total.shape[2] // 2
        send = total[:, :, half:].astype(BF16)
        arrived = swap(send, "pulse", 1 << stage)
        for p in parts:
            halves[p] = None
        halves[parts[-1]] = (total[:, :, :half], arrived, stages)
        return send

    for part in range(calls):
        done = []
        for p in range(part - 1):
            if halves[p] is None or halves[p][2] == stages:
                continue
            if calls == 5 and stages == 3 and p == 0 and part == 3:
                continue
            if calls == 5 and stages == 3 and p == 0 and part == 4:
                done.append(advance_together([0, 1]))
            else:
                done.append(advance(p))
        if done:
            phase, done = lax.optimization_barrier((phase, done))
        keep, send, phase, *ahead = partial_spectrum(
            here, there, tables, phase, pulse_data, other,
            sum(sizes[: part + 1]) * LANES,
            sizes[part + 1] if part + 1 < calls else 0,
            classes,
        )
        if ahead:
            here, there = ahead
        halves[part] = (keep, swap(send, "pulse", 1), 1)
    for stage in range(1, stages):
        for part in range(calls):
            if halves[part] is not None and halves[part][2] == stage:
                advance(part)
    kept = [half[0] for half in halves if half is not None]
    received = [half[1] for half in halves if half is not None]
    spectrum, cov = spectrum_and_covariance(kept, received, angles ** (-0.5))
    covs = [cov]
    distance = 1
    while distance < range_count:
        total = covs[0]
        for extra in covs[1:]:
            total = total + extra
        covs = [total]
        for turn in range(1, min(4, range_count // distance)):
            covs.append(swap(total, "range", turn * distance))
        distance *= 4
    return focus(covs, spectrum)


def solution(mesh):
    placed = (
        P(None, "pulse", "range"),
        P(None, None, None, "pulse"),
        P(None, None, None, "pulse"),
        P(None, "pulse"),
    )
    return jax.shard_map(
        per_device, mesh=mesh, in_specs=placed, out_specs=P(None, "pulse", "range"), check_vma=False
    )
```

```python
import functools
import math

import jax
import jax.numpy as jnp
from jax import lax
from jax.experimental import pallas as pl
from jax.experimental.pallas import tpu as pltpu
from jax.sharding import PartitionSpec as P


BINS = 1024
BLOCK = 64
POWER = 3
MIB = 1024 * 1024
SMALL_LIMIT = 4
LANES = 128
EPSILON = 1e-06


F32 = jnp.float32
BF16 = jnp.bfloat16


SINE = (3.1415926401307077, -5.16771008350789, 2.550077523214589, -0.5982912856206265, 0.07765766030630428)
COSINE = (0.9999999532476085, -4.934792830619644, 4.058411352862619, -1.3318765680811142, 0.2196896110983216)


def cis_turns(turns):
    z = turns - jnp.floor(turns + 0.5)
    w = z * z
    s, c = SINE[-1], COSINE[-1]
    for more in SINE[-2::-1]:
        s = s * w + more
    for more in COSINE[-2::-1]:
        c = c * w + more
    s = s * z
    twice = s + s
    return 1.0 - twice * s, twice * c


def swap(block, axis, distance):
    count = lax.axis_size(axis)
    return lax.ppermute(block, axis, [(i, i ^ distance) for i in range(count)])


VMEM = pl.BlockSpec(memory_space=pltpu.VMEM)
SMEM = pl.BlockSpec(memory_space=pltpu.SMEM)
HBM = pl.BlockSpec(memory_space=pltpu.HBM)


def pack_kernel(taps, weights, squint, mine, near, far):
    def put(out, row, level, source):
        out[row : row + 4] = taps[level, source].astype(F32)
        out[row + 4 : row + 8] = weights[level, source].astype(F32)

    put(mine, 0, 0, 0)
    put(mine, 8, 0, 1)
    put(mine, 16, 1, 0)
    put(mine, 24, 2, 0)
    mine[32:35] = squint[...]
    mine[35:40] = jnp.zeros((5, mine.shape[1]), F32)
    put(near, 0, 1, 1)
    put(near, 8, 2, 0)
    near[16:19] = squint[...]
    near[19:24] = jnp.zeros((5, near.shape[1]), F32)
    put(far, 0, 2, 1)
    far[8:11] = squint[...]
    far[11:16] = jnp.zeros((5, far.shape[1]), F32)


def pack(taps, weights, squint):
    beams = squint.shape[1]
    return pl.pallas_call(
        pack_kernel,
        in_specs=[VMEM] * 3,
        out_specs=[VMEM] * 3,
        out_shape=[jax.ShapeDtypeStruct((rows, beams), F32) for rows in (40, 24, 16)],
        compiler_params=pltpu.CompilerParams(vmem_limit_bytes=SMALL_LIMIT * MIB),
        name="pack",
    )(taps, weights, squint)


def fill_matrices(columns, outs):
    beams = columns.shape[0]

    def part(i, _):
        at = pl.ds(pl.multiple_of(i * 16, 16), 16)
        lane = lax.broadcasted_iota(jnp.int32, (16, LANES), 1)
        lanes = [(lane + j * LANES).astype(jnp.int16) for j in range(beams // LANES)]
        whole = columns[at, :].astype(jnp.int32).astype(jnp.int16)
        real = columns[at, :].astype(BF16)

        def spread(value, column):
            return jnp.broadcast_to(value[:, column : column + 1], (16, LANES))

        for unit, out in enumerate(outs):
            taps = [spread(whole, 8 * unit + c) for c in range(4)]
            weights = [spread(real, 8 * unit + 4 + c) for c in range(4)]
            for j, here in enumerate(lanes):
                total = jnp.zeros((16, LANES), BF16)
                for tap, weight in zip(taps, weights):
                    total = jnp.where(here == tap, weight, total)
                out[at, j * LANES : (j + 1) * LANES] = total
        return 0

    lax.fori_loop(0, beams // 16, part, 0, unroll=2)


def first_kernel(pulses, scalars, mine, matrices, table, columns, rows):
    beams = matrices.shape[1]
    angles = beams * pulses
    classes = pulses // 2
    each = BINS // pulses
    rows[0:40] = mine[...]
    columns[...] = rows[...].T
    fill_matrices(columns, [matrices.at[u] for u in range(2)])
    count = BINS // classes
    inner = each // classes
    bits = pulses.bit_length() - 1

    def part(i, _):
        at = pl.ds(pl.multiple_of(i * 16, 16), 16)
        row = lax.broadcasted_iota(jnp.int32, (16, LANES), 0) + i * 16
        group = (row & (count - 1)) >> (inner.bit_length() - 1)
        mirrored = jnp.zeros_like(group)
        for bit in range(bits):
            mirrored = mirrored | ((group >> bit & 1) << (bits - 1 - bit))
        bins = (
            (mirrored ^ scalars[0]) * each
            + (row & (inner - 1)) * classes
            + (row >> (count.bit_length() - 1))
        )
        lane = lax.broadcasted_iota(jnp.int32, (16, LANES), 1)
        whole = angles - 1
        cosine, sine = cis_turns(
            (bins * (scalars[2] + lane & whole) & whole).astype(F32) * (1.0 / angles)
        )
        ahead_c, ahead_s = cis_turns((bins * LANES & whole).astype(F32) * (1.0 / angles))
        low = i * 16 + (i * 16 >> (count.bit_length() - 1)) * count
        cos_at = pl.ds(pl.multiple_of(low, 16), 16)
        sin_at = pl.ds(pl.multiple_of(low + count, 16), 16)
        for j in range(beams // LANES):
            lanes = slice(j * LANES, (j + 1) * LANES)
            table[cos_at, lanes] = cosine.astype(BF16)
            table[sin_at, lanes] = sine.astype(BF16)
            cosine, sine = (
                cosine * ahead_c - sine * ahead_s,
                sine * ahead_c + cosine * ahead_s,
            )
        return 0

    lax.fori_loop(0, BINS // 16, part, 0, unroll=4)


def first_tables(scalars, mine, pulses):
    beams = mine.shape[1]
    return pl.pallas_call(
        functools.partial(first_kernel, pulses),
        in_specs=[SMEM, VMEM],
        out_specs=[VMEM] * 2,
        out_shape=[
            jax.ShapeDtypeStruct((2, beams, beams), BF16),
            jax.ShapeDtypeStruct((2 * BINS, beams), BF16),
        ],
        scratch_shapes=[pltpu.VMEM((beams, LANES), F32), pltpu.VMEM((LANES, beams), F32)],
        compiler_params=pltpu.CompilerParams(vmem_limit_bytes=SMALL_LIMIT * MIB),
        cost_estimate=pl.CostEstimate(
            flops=4000 * beams * beams, bytes_accessed=8 * beams * beams, transcendentals=0
        ),
        name="first",
    )(scalars, mine)


def fetch(pulse_data, other, here, there, sems, start):
    return [
        pltpu.make_async_copy(
            source.at[t, :, pl.ds(start + j * LANES, LANES)],
            to.at[j, :, pl.ds(t * LANES, LANES)],
            sems.at[i, j, t],
        )
        for i, (source, to) in enumerate(((pulse_data, here), (other, there)))
        for j in range(here.shape[0])
        for t in range(2)
    ]


def second_kernel(
    ranges,
    scalars, mine, near, middle, far, pulse_data, other,
    split, join, phase, step, here, there,
    columns, rows, packs, sems,
):
    copies = fetch(pulse_data, other, here, there, sems, 0)
    for copy in copies:
        copy.start()
    beams = split.shape[1]
    place = scalars[1]
    packs[0, 0:8] = mine[24:32]
    packs[0, 8:16] = jnp.broadcast_to(mine[34:35], (8, beams))
    packs[1, 0:8] = near[8:16]
    packs[1, 8:16] = jnp.broadcast_to(near[18:19], (8, beams))
    packs[2, 0:8] = middle[0:8]
    packs[2, 8:16] = jnp.broadcast_to(middle[10:11], (8, beams))
    packs[3, 0:8] = far[0:8]
    packs[3, 8:16] = jnp.broadcast_to(far[10:11], (8, beams))
    packs[4, 0:8] = mine[16:24]
    packs[4, 8:16] = jnp.broadcast_to(mine[33:34], (8, beams))
    packs[5, 0:8] = near[0:8]
    packs[5, 8:16] = jnp.broadcast_to(near[17:18], (8, beams))
    order = [4 + (x ^ place & 1) for x in range(2)] + [k ^ place for k in range(4)]
    rows[48:56] = jnp.broadcast_to(mine[32:33], (8, beams))
    for unit, source in enumerate(order):
        rows[8 * unit : 8 * unit + 8] = packs[source, 0:8]
        rows[56 + 8 * unit : 64 + 8 * unit] = packs[source, 8:16]
    columns[...] = rows[...].T
    fill_matrices(
        columns, [split.at[u] for u in range(2)] + [join.at[u] for u in range(4)]
    )

    def part(i, _):
        at = pl.ds(pl.multiple_of(i * 16, 16), 16)
        p = columns[at, :]
        lane = lax.broadcasted_iota(jnp.int32, (16, LANES), 1)
        index = (lane + scalars[3]).astype(F32) * (1.0 / ranges)
        for unit in range(7):
            squint = p[:, 48 + 8 * unit : 49 + 8 * unit]
            cosine, sine = cis_turns(squint * index)
            phase[unit, 0, at, :] = cosine
            phase[unit, 1, at, :] = sine
        cosine, sine = cis_turns(p * (LANES / ranges))
        step[0, at, :] = cosine
        step[1, at, :] = sine
        return 0

    lax.fori_loop(0, beams // 16, part, 0, unroll=4)
    for copy in copies:
        copy.wait()


def second_tables(scalars, mine, near, middle, far, pulse_data, other, ranges, chunks):
    beams = mine.shape[1]
    return pl.pallas_call(
        functools.partial(second_kernel, ranges),
        in_specs=[SMEM] + [VMEM] * 4 + [HBM] * 2,
        out_specs=[VMEM] * 6,
        out_shape=[
            jax.ShapeDtypeStruct((2, beams, beams), BF16),
            jax.ShapeDtypeStruct((4, beams, beams), BF16),
            jax.ShapeDtypeStruct((7, 2, beams, LANES), F32),
            jax.ShapeDtypeStruct((2, beams, LANES), F32),
            jax.ShapeDtypeStruct((chunks, beams, 2 * LANES), BF16),
            jax.ShapeDtypeStruct((chunks, beams, 2 * LANES), BF16),
        ],
        scratch_shapes=[
            pltpu.VMEM((beams, LANES), F32),
            pltpu.VMEM((LANES, beams), F32),
            pltpu.VMEM((6, 16, beams), F32),
            pltpu.SemaphoreType.DMA((2, chunks, 2)),
        ],
        compiler_params=pltpu.CompilerParams(vmem_limit_bytes=SMALL_LIMIT * MIB),
        cost_estimate=pl.CostEstimate(
            flops=8000 * beams * beams, bytes_accessed=12 * beams * beams, transcendentals=0
        ),
        name="second",
    )(scalars, mine, near, middle, far, pulse_data, other)


def turned(base, value, turn, count):
    c = math.cos(2.0 * math.pi * turn / count)
    s = math.sin(2.0 * math.pi * turn / count)
    real, imag = base
    re, im = value
    for amount, add_re, add_im in ((c, re, im), (s, im, -re)):
        if abs(amount) < 1e-9:
            continue
        if abs(abs(amount) - 1.0) > 1e-9:
            real, imag = real + amount * add_re, imag + amount * add_im
        elif amount > 0.0:
            real, imag = real + add_re, imag + add_im
        else:
            real, imag = real - add_re, imag - add_im
    return real, imag


def main_limit(classes):
    return (7 if classes <= 4 else 40) * MIB


def main_kernel(
    start, classes, more,
    near, far, merge, split, join, azimuth, step, phase_in,
    *refs,
):
    if more:
        pulse_data, other, keep, send, phase, here, there, merged, pair, spread, sems = refs
        copies = fetch(pulse_data, other, here, there, sems, start)
    else:
        keep, send, phase, merged, pair, spread = refs
        copies = []
    for copy in copies:
        copy.start()
    beams = merged.shape[0]
    tile = 512
    tiles = beams // tile
    small = 256

    def rotate(unit, at, total):
        cosine = phase[unit, 0, at, :]
        sine = phase[unit, 1, at, :]
        if more or near.shape[0] > 1:
            ahead_c = step[0, at, 48 + 8 * unit : 49 + 8 * unit]
            ahead_s = step[1, at, 48 + 8 * unit : 49 + 8 * unit]
            phase[unit, 0, at, :] = cosine * ahead_c - sine * ahead_s
            phase[unit, 1, at, :] = cosine * ahead_s + sine * ahead_c
        real = total[:, :LANES]
        imag = total[:, LANES:]
        return cosine * real - sine * imag, sine * real + cosine * imag

    def product(lhs, rhs):
        return jnp.dot(lhs, rhs, preferred_element_type=F32)

    def chunk(j, _):
        lanes = pl.ds(pl.multiple_of(j * LANES, LANES), LANES)
        for i in range(tiles):
            at = pl.ds(i * tile, tile)
            real, imag = rotate(
                0, at, product(merge[0, at, :], near[j]) + product(merge[1, at, :], far[j])
            )
            merged[at, :LANES] = real.astype(BF16)
            merged[at, LANES:] = imag.astype(BF16)
        for x in range(2):
            for i in range(tiles):
                at = pl.ds(i * tile, tile)
                real, imag = rotate(1 + x, at, product(split[x, at, :], merged[...]))
                pair[x, at, :LANES] = real.astype(BF16)
                pair[x, at, LANES:] = imag.astype(BF16)
        for i in range(beams // small):
            at = pl.ds(i * small, small)
            terms = [
                rotate(3 + k, at, product(join[k, at, :], pair[k % 2])) for k in range(4)
            ]
            pairs = {}
            for q in range(classes):
                turn = 2 * q % classes
                if turn not in pairs:
                    pairs[turn] = [turned(terms[x], terms[x + 2], turn, classes) for x in range(2)]
                real, imag = turned(*pairs[turn], q, classes)
                spread[q, at, :LANES] = real.astype(BF16)
                spread[q, at, LANES:] = imag.astype(BF16)
        rows = BINS // classes
        half = rows // 2
        for q in range(classes):
            both = product(azimuth[pl.ds(2 * q * rows, 2 * rows), :], spread[q])
            by_cos, by_sin = both[:rows], both[rows:]
            sides = (
                by_cos[:, :LANES] + by_sin[:, LANES:],
                by_cos[:, LANES:] - by_sin[:, :LANES],
            )
            for t, side in enumerate(sides):
                keep[t, q, :, lanes] = side[:half]
                send[t, q, :, lanes] = side[half:].astype(BF16)
        return 0

    lax.fori_loop(0, near.shape[0], chunk, 0)
    for copy in copies:
        copy.wait()


def partial_spectrum(near, far, tables, phase, pulse_data, other, start, chunks, classes):
    beams = near.shape[1]
    width = near.shape[0] * LANES
    half = BINS // classes // 2
    ahead = [jax.ShapeDtypeStruct((chunks, beams, 2 * LANES), BF16)] * 2 if chunks else []
    return pl.pallas_call(
        functools.partial(main_kernel, start, classes, chunks > 0),
        in_specs=[VMEM] * 8 + [HBM] * len(ahead),
        out_specs=[VMEM] * (3 + len(ahead)),
        out_shape=[
            jax.ShapeDtypeStruct((2, classes, half, width), F32),
            jax.ShapeDtypeStruct((2, classes, half, width), BF16),
            jax.ShapeDtypeStruct(phase.shape, F32),
        ]
        + ahead,
        scratch_shapes=[
            pltpu.VMEM((beams, 2 * LANES), BF16),
            pltpu.VMEM((2, beams, 2 * LANES), BF16),
            pltpu.VMEM((classes, beams, 2 * LANES), BF16),
        ]
        + ([pltpu.SemaphoreType.DMA((2, chunks, 2))] if ahead else []),
        input_output_aliases={7: 2},
        compiler_params=pltpu.CompilerParams(vmem_limit_bytes=main_limit(classes)),
        cost_estimate=pl.CostEstimate(
            flops=2 * 20 * beams * beams * width,
            bytes_accessed=beams * beams,
            transcendentals=0,
        ),
        name="main",
    )(near, far, *tables, phase, *([pulse_data, other] if ahead else []))


def covariance_kernel(scale, *refs):
    parts = (len(refs) - 2) // 2
    kept, received = refs[:parts], refs[parts : 2 * parts]
    spectrum, covariance = refs[2 * parts :]
    classes, rows = kept[0].shape[1:3]
    inner = BLOCK // classes
    at = 0
    for h in range(parts):
        width = kept[h].shape[3]
        spectrum[:, :, :, at : at + width] = (
            kept[h][...] + received[h][...].astype(F32)
        ) * scale
        at += width

    def gram(a, b):
        return lax.dot_general(
            a, b, (((1,), (1,)), ((), ())),
            precision=lax.Precision.HIGHEST, preferred_element_type=F32,
        )

    def block(b, _):
        at = pl.ds(pl.multiple_of(b * inner, inner), inner)
        real, imag = [
            jnp.concatenate([spectrum[t, q, at, :] for q in range(classes)], axis=0)
            for t in range(2)
        ]
        covariance[b] = gram(real, jnp.concatenate([real, -imag], axis=0)) + gram(
            imag, jnp.concatenate([imag, real], axis=0)
        )
        return 0

    lax.fori_loop(0, rows // inner, block, 0)


def spectrum_and_covariance(kept, received, scale):
    _, classes, rows, _ = kept[0].shape
    width = sum(part.shape[3] for part in kept)
    inner = BLOCK // classes
    return pl.pallas_call(
        functools.partial(covariance_kernel, scale),
        in_specs=[VMEM] * (2 * len(kept)),
        out_specs=[VMEM, VMEM],
        out_shape=[
            jax.ShapeDtypeStruct((2, classes, rows, width), F32),
            jax.ShapeDtypeStruct((rows // inner, BLOCK, 2 * BLOCK), F32),
        ],
        compiler_params=pltpu.CompilerParams(vmem_limit_bytes=SMALL_LIMIT * MIB),
        name="covariance",
    )(*kept, *received)


def focus_kernel(*refs):
    covs, (spectrum, out, stage) = refs[:-3], refs[-3:]
    classes, rows = spectrum.shape[1:3]
    inner = BLOCK // classes
    factor = math.sqrt(BLOCK)
    lane = lax.broadcasted_iota(jnp.int32, (1, 2 * BLOCK), 1)
    first = lane < BLOCK

    def turned(row):
        return pltpu.roll(jnp.broadcast_to(row, (8, 2 * BLOCK)), BLOCK, 1)[0:1]

    for b in range(rows // inner):
        cov = covs[0][b]
        for other in covs[1:]:
            cov = cov + other[b]
        vec_re = jnp.where(first, 1.0, 0.0)
        vec_im = jnp.zeros((1, 2 * BLOCK), F32)
        for step in range(POWER):
            if step % 2 == 0:
                new_re = jnp.sum(
                    cov * jnp.where(first, vec_re, -turned(vec_im)), axis=1, keepdims=True
                )
                new_im = jnp.sum(
                    cov * jnp.where(first, vec_im, turned(vec_re)), axis=1, keepdims=True
                )
                power = jnp.sum(new_re * new_re + new_im * new_im, axis=0, keepdims=True)
            else:
                by_re = jnp.sum(cov * vec_re, axis=0, keepdims=True)
                by_im = jnp.sum(cov * vec_im, axis=0, keepdims=True)
                new_re = jnp.where(first, by_re + turned(by_im), 0.0)
                new_im = jnp.where(first, by_im - turned(by_re), 0.0)
                power = jnp.sum(new_re * new_re + new_im * new_im, axis=1, keepdims=True)
            length = jnp.sqrt(power + EPSILON)
            vec_re = new_re / length
            vec_im = new_im / length
        for q in range(classes):
            re = spectrum[0, q, b * inner : (b + 1) * inner, :]
            im = spectrum[1, q, b * inner : (b + 1) * inner, :]
            by_re = vec_re[q * inner : (q + 1) * inner] * factor
            by_im = vec_im[q * inner : (q + 1) * inner] * factor
            at = pl.ds(q, inner, stride=classes)
            for t, side in enumerate((re * by_re + im * by_im, im * by_re - re * by_im)):
                for j in range(stage.shape[1]):
                    stage[t, j, at, :] = side[:, j * LANES : (j + 1) * LANES]
        for t in range(2):
            for j in range(stage.shape[1]):
                out[t, b * BLOCK : (b + 1) * BLOCK, j * LANES : (j + 1) * LANES] = stage[t, j]


def focus(covs, spectrum):
    _, classes, rows, ranges = spectrum.shape
    return pl.pallas_call(
        focus_kernel,
        in_specs=[VMEM] * (len(covs) + 1),
        out_specs=VMEM,
        out_shape=jax.ShapeDtypeStruct((2, classes * rows, ranges), F32),
        scratch_shapes=[pltpu.VMEM((2, ranges // LANES, BLOCK, LANES), F32)],
        compiler_params=pltpu.CompilerParams(vmem_limit_bytes=SMALL_LIMIT * MIB),
        name="focus",
    )(*covs, spectrum)


def per_device(pulse_data, merge_taps, merge_weights, squint):
    pulses = lax.axis_size("pulse")
    range_count = lax.axis_size("range")
    pulse_index = lax.axis_index("pulse")
    range_index = lax.axis_index("range")
    _, beams, range_cols = pulse_data.shape
    ranges = range_cols * range_count
    angles = beams * pulses
    classes = pulses // 2
    mine, near, far = pack(merge_taps, merge_weights, squint)
    near = swap(near, "pulse", 2)
    middle = swap(far, "pulse", 4)
    far = swap(far, "pulse", 6)
    other = swap(pulse_data, "pulse", 1)
    scalars = jnp.stack(
        [
            pulse_index,
            pulse_index >> 1 & 3,
            (pulse_index & ~6) * beams,
            range_index * range_cols,
        ]
    )
    merge, azimuth = first_tables(scalars, mine, pulses)
    total = range_cols // LANES
    sizes = [total // 4, total // 4, total // 4, total - total // 8 * 7, total // 8] if total >= 8 else [1] * total
    calls = len(sizes)
    split, join, phase, step, here, there = second_tables(
        scalars, mine, near, middle, far, pulse_data, other, ranges, sizes[0]
    )
    tables = (merge, split, join, azimuth, step)
    stages = pulses.bit_length() - 1
    halves = [None] * calls

    def advance(part):
        keep, arrived, stage = halves[part]
        total = keep + arrived.astype(F32)
        half = total.shape[2] // 2
        send = total[:, :, half:].astype(BF16)
        arrived = swap(send, "pulse", 1 << stage)
        halves[part] = (total[:, :, :half], arrived, stage + 1)
        return send

    for part in range(calls):
        done = [advance(p) for p in range(part - 1) if halves[p][2] < stages]
        if done:
            phase, done = lax.optimization_barrier((phase, done))
        keep, send, phase, *ahead = partial_spectrum(
            here, there, tables, phase, pulse_data, other,
            sum(sizes[: part + 1]) * LANES,
            sizes[part + 1] if part + 1 < calls else 0,
            classes,
        )
        if ahead:
            here, there = ahead
        halves[part] = (keep, swap(send, "pulse", 1), 1)
    for stage in range(1, stages):
        for part in range(calls):
            if halves[part][2] == stage:
                advance(part)
    kept = [half[0] for half in halves]
    received = [half[1] for half in halves]
    spectrum, cov = spectrum_and_covariance(kept, received, angles ** (-0.5))
    covs = [cov]
    distance = 1
    while distance < range_count:
        total = covs[0]
        for extra in covs[1:]:
            total = total + extra
        covs = [total]
        for turn in range(1, min(4, range_count // distance)):
            covs.append(swap(total, "range", turn * distance))
        distance *= 4
    return focus(covs, spectrum)


def solution(mesh):
    placed = (
        P(None, "pulse", "range"),
        P(None, None, None, "pulse"),
        P(None, None, None, "pulse"),
        P(None, "pulse"),
    )
    return jax.shard_map(
        per_device, mesh=mesh, in_specs=placed, out_specs=P(None, "pulse", "range"), check_vma=False
    )
```
